128 devices in a mesh: ctx: 16 (over y, z), head: 8 (over x, core).
Axes of the slice: x: 4, y: 4, z: 4, core: 2. Of those that a mesh axis runs over, the one named last changes fastest.
Arguments:
- queries: bfloat16 [16384, 2048], P('ctx', 'head'), may hold values from -6 to 6
- keys: bfloat16 [16384, 2048], P('ctx', 'head'), may hold values from -1.7 to 1.7
- values: bfloat16 [16384, 2048], P('ctx', 'head'), may hold values from -6 to 6
- w_out: bfloat16 [2048, 2048], P('head'), may hold values from -0.125 to 0.125
- cotangent: bfloat16 [16384, 2048], P('ctx', 'head'), may hold values from -6 to 6
Outputs:
- layer_out: bfloat16 [16384, 2048], P('ctx', 'head')
- grad_queries: bfloat16 [16384, 2048], P('ctx', 'head')
- grad_keys: bfloat16 [16384, 2048], P('ctx', 'head')
- grad_values: bfloat16 [16384, 2048], P('ctx', 'head')
- grad_weight: float32 [2048, 2048], P('head', 'ctx')
The draws below stay inside these ranges and needn't reach their ends.
All inputs are finite; a program needn't handle non-finite values.
Results may differ from the reference program's by a relative error of at most 0.014.
Values may be sent and summed in bfloat16 or wider, within the bound.
A program may use at most 128 MiB of HBM per device.

```python
import jax
import jax.numpy as jnp
from jax import lax

HDIM = 128
D = 2048
SPAN = 256
NEWTON = 8
HEADS = 16
TOKENS = 16384


def draw_keys(key, part):
    scale_key, entry_key = jax.random.split(jax.random.fold_in(key, 11))
    columns = HEADS * HDIM
    spread = jax.random.uniform(scale_key, (columns,), jnp.float32, -2.5, 2.5)
    entries = jax.random.truncated_normal(entry_key, -6.0, 6.0, (TOKENS, columns), jnp.float32)
    return (0.023 * jnp.exp(spread)[None, :] * entries).astype(jnp.bfloat16)


def block_scale(rng, shape, cuts, least, top_value):
    level = 1.0
    for position, blocks in cuts:
        draws = jax.random.uniform(jax.random.fold_in(jax.random.fold_in(rng, 6), position), (blocks,), jnp.float32, least / len(cuts), top_value / len(cuts))
        level = level * jnp.repeat(jnp.exp(draws), shape[position] // blocks).reshape((-1,) + (1,) * (len(shape) - 1 - position))
    return level


def centred(stream_key, shape, width, limit, cuts=(), kind=jnp.bfloat16):
    result = width * jax.random.normal(stream_key, shape, jnp.float32)
    if cuts:
        result = result * block_scale(stream_key, shape, cuts, -0.22, 0.18)
    return jnp.clip(result, -limit, limit).astype(kind)


def setup_inputs(seed: int = 0) -> dict:
    streams_of = jax.random.split(jax.random.key(seed), 6)
    return {
        "queries": centred(streams_of[0], (TOKENS, HEADS * HDIM), 1.0, 6.0, ((0, 16), (1, 8))),
        "keys": draw_keys(jax.random.fold_in(streams_of[5], 71), 0),
        "values": centred(streams_of[2], (TOKENS, HEADS * HDIM), 1.0, 6.0, ((0, 16), (1, 8))),
        "w_out": centred(streams_of[3], (HEADS * HDIM, D), (HEADS * HDIM) ** -0.5, 0.125, ((0, 8),)),
        "cotangent": centred(streams_of[4], (TOKENS, D), 1.0, 6.0, ((0, 16), (1, 8))),
    }


RIDGE = 1.0
HIGH = lax.Precision.HIGHEST

def newton_inverse(matrix):
    size = matrix.shape[0]
    unit_matrix = jnp.eye(size, dtype=jnp.float32)
    approx = unit_matrix / jnp.sqrt(jnp.sum(matrix * matrix))
    for step in range(NEWTON):
        product = jnp.dot(matrix, approx, precision=HIGH)
        approx = jnp.dot(approx, 2.0 * unit_matrix - product, precision=HIGH)
    return approx

def block_output(block_q, block_k, block_v, gram, memory):
    size = gram.shape[0]
    ridged = gram + RIDGE * jnp.eye(size, dtype=jnp.float32)
    inverse = newton_inverse(ridged)
    solved = jnp.dot(block_q, inverse, precision=HIGH)
    scores = jnp.dot(solved, block_k.T, precision=HIGH)
    length = scores.shape[0]
    causal = jnp.arange(length)[:, None] >= jnp.arange(length)[None, :]
    scores = jnp.where(causal, scores, jnp.zeros_like(scores))
    return jnp.dot(scores, block_v, precision=HIGH) + jnp.dot(solved, memory.T, precision=HIGH)

def exclusive_forward(blocks):
    running = jnp.cumsum(blocks, axis=0)
    return jnp.concatenate([jnp.zeros_like(blocks[:1]), running[:-1]], axis=0)

def exclusive_backward(blocks):
    running = jnp.cumsum(blocks[::-1], axis=0)[::-1]
    return jnp.concatenate([running[1:], jnp.zeros_like(blocks[:1])], axis=0)

def head_pass(stacked):
    head_q, head_k, head_v, head_grad = stacked
    blocks = head_q.shape[0] // SPAN
    q_float = head_q.astype(jnp.float32).reshape(blocks, SPAN, HDIM)
    k_float = head_k.astype(jnp.float32).reshape(blocks, SPAN, HDIM)
    v_float = head_v.astype(jnp.float32).reshape(blocks, SPAN, HDIM)
    grams = jnp.einsum('cti,ctj->cij', k_float, k_float, precision=HIGH)
    pairs = jnp.einsum('cti,ctj->cij', v_float, k_float, precision=HIGH)
    gram_prefix = exclusive_forward(grams)
    pair_prefix = exclusive_forward(pairs)
    outputs, pullback = jax.vjp(jax.vmap(block_output), q_float, k_float, v_float, gram_prefix, pair_prefix)
    grad_out = head_grad.astype(jnp.float32).reshape(blocks, SPAN, HDIM)
    d_query, d_key, d_value, d_gram, d_pair = pullback(grad_out)
    gram_suffix = exclusive_backward(d_gram)
    pair_suffix = exclusive_backward(d_pair)
    symmetric = gram_suffix + jnp.swapaxes(gram_suffix, 1, 2)
    d_key = d_key + jnp.einsum('cti,cij->ctj', k_float, symmetric, precision=HIGH)
    d_key = d_key + jnp.einsum('cti,cij->ctj', v_float, pair_suffix, precision=HIGH)
    d_value = d_value + jnp.einsum('ctj,cij->cti', k_float, pair_suffix, precision=HIGH)
    shape = (blocks * SPAN, HDIM)
    return (outputs.reshape(shape).astype(jnp.bfloat16), d_query.reshape(shape).astype(jnp.bfloat16), d_key.reshape(shape).astype(jnp.bfloat16), d_value.reshape(shape).astype(jnp.bfloat16))

def by_head(array):
    return array.reshape(TOKENS, HEADS, HDIM).transpose(1, 0, 2)

def from_head(array):
    return array.transpose(1, 0, 2).reshape(TOKENS, HEADS * HDIM)

def reference(queries, keys, values, w_out, cotangent):
    grad_heads = jnp.dot(cotangent, w_out.T, preferred_element_type=jnp.float32).astype(jnp.bfloat16)
    results = lax.map(head_pass, (by_head(queries), by_head(keys), by_head(values), by_head(grad_heads)))
    heads_out = from_head(results[0])
    layer_out = jnp.dot(heads_out, w_out, preferred_element_type=jnp.float32).astype(jnp.bfloat16)
    grad_weight = jnp.dot(heads_out.T, cotangent, preferred_element_type=jnp.float32)
    return (layer_out, from_head(results[1]), from_head(results[2]), from_head(results[3]), grad_weight)
```

```python
import jax
import jax.numpy as jnp
from jax import lax
from jax.experimental import pallas as pl
from jax.experimental.pallas import tpu as pltpu
from jax.sharding import PartitionSpec as P

HDIM = 128
SPAN = 256
NEWTON = 8
RIDGE = 1.0
NB = 4
NH = 2
NP = NB * NH
CTX = 16
CHIPS = 4
F32 = jnp.float32
BF = jnp.bfloat16
MESH = pl.DeviceIdType.MESH


def mm(a, b):
    return lax.dot_general(a, b, (((1,), (0,)), ((), ())), preferred_element_type=F32)


def mm_nt(a, b):
    return lax.dot_general(a, b, (((1,), (1,)), ((), ())), preferred_element_type=F32)


def mm_tn(a, b):
    return lax.dot_general(a, b, (((0,), (0,)), ((), ())), preferred_element_type=F32)


def rows(*parts):
    return jnp.concatenate(parts, axis=0)


def lanes(*parts):
    return jnp.concatenate(parts, axis=1)


def halves(value):
    high = value.astype(BF)
    return high, (value - high.astype(F32)).astype(BF)


def total(value):
    return jnp.sum(jnp.sum(value, axis=1, keepdims=True), axis=0, keepdims=True)


def eye():
    shape = (HDIM, HDIM)
    return (
        lax.broadcasted_iota(jnp.int32, shape, 0) == lax.broadcasted_iota(jnp.int32, shape, 1)
    ).astype(F32)


def causal(value):
    shape = (SPAN, SPAN)
    keep = lax.broadcasted_iota(jnp.int32, shape, 0) >= lax.broadcasted_iota(jnp.int32, shape, 1)
    return jnp.where(keep, value, 0.0)


def kernel(
    q_ref, k_ref, v_ref, w_ref, cot_ref,
    lo_ref, gq_ref, gk_ref, gv_ref, gw_ref,
    ag, st, inbox, outb, off, st2, inbox2, outb2, off2,
    gram_s, pair_s, exh, exl, dth, dtl, scale_s, mem_h, mem_l,
    sol_h, sol_l, sc_h, sc_l, ho, hot, do, dk_s, dv_s, dg_s, dm_s,
    d2o, d2i, x2o, x2i, xpo, xmo, xli, xri, loacc, wt, gwi,
    ag_s, ag_r, sc1_s, sc1_r, sc2_s, sc2_r, sc3_s, sc3_r, sc4_s, sc4_r,
    gw_s, gw_r, d2_s, d2_r, x2_s, x2_r, xp_s, xp_r, xm_s, xm_r,
):
    me = lax.axis_index("ctx")
    hd = lax.axis_index("head")
    x = lax.div(hd, 2)
    core = lax.rem(hd, 2)
    right = lax.rem(x + 1, CHIPS) * 2 + core
    left = lax.rem(x + 3, CHIPS) * 2 + core
    far = lax.rem(x + 2, CHIPS) * 2 + core
    twin = x * 2 + 1 - core
    sent = []

    def remote(src, dst, ss, rs, dev):
        return pltpu.make_async_remote_copy(
            src_ref=src, dst_ref=dst, send_sem=ss, recv_sem=rs, device_id=dev, device_id_type=MESH
        )

    def push(src, dst, ss, rs, dev):
        copy = remote(src, dst, ss, rs, dev)
        copy.start()
        sent.append(copy)

    def arrived(dst, ss, rs):
        remote(dst, dst, ss, rs, (me, twin)).wait_recv()

    def exchange(src, dst, ss, rs):
        for d in range(1, CTX):
            peer = lax.rem(me + d, CTX)
            push(src.at[peer], dst.at[me], ss.at[d - 1], rs.at[d - 1], (peer, hd))
        dst[me] = src[me]

    def exchanged(dst, ss, rs):
        for d in range(1, CTX):
            peer = lax.rem(me + CTX - d, CTX)
            arrived(dst.at[peer], ss.at[d - 1], rs.at[d - 1])

    def rows_of(b):
        return pl.ds(pl.multiple_of(b * SPAN, SPAN), SPAN)

    def cols_of(h):
        return slice(h * HDIM, (h + 1) * HDIM)

    barrier = pltpu.get_barrier_semaphore()
    for d in range(1, CTX):
        pl.semaphore_signal(barrier, inc=1, device_id=(lax.rem(me + d, CTX), hd), device_id_type=MESH)
    for dev in (right, left, twin):
        pl.semaphore_signal(barrier, inc=1, device_id=(me, dev), device_id_type=MESH)
    pl.semaphore_wait(barrier, CTX - 1 + 3)

    for b in range(NB):
        for kind, dev, blk in ((0, right, b), (1, left, (b + 2) % NB)):
            push(
                cot_ref.at[pl.ds(blk * SPAN, SPAN), :], ag.at[hd, blk],
                ag_s.at[kind, blk], ag_r.at[kind, blk], (me, dev),
            )
    for b in range(NB):
        push(
            cot_ref.at[pl.ds(b * SPAN, SPAN), :], ag.at[hd, b],
            ag_s.at[3, b], ag_r.at[3, b], (me, twin),
        )
        ag[hd, b] = cot_ref[b * SPAN : (b + 1) * SPAN, :]

    def take(kind, b, relay=None):
        shard = (left, right, far)[kind]
        here = ag.at[shard, b]
        arrived(here, ag_s.at[kind, b], ag_r.at[kind, b])
        if relay is not None:
            push(here, here, ag_s.at[2, b], ag_r.at[2, b], (me, relay))
        push(here, here, ag_s.at[4 + kind, b], ag_r.at[4 + kind, b], (me, twin))

    for h in range(NH):
        gram_sum = jnp.zeros((HDIM, HDIM), F32)
        pair_sum = jnp.zeros((HDIM, HDIM), F32)
        for b in range(NB):
            kb = k_ref[b * SPAN : (b + 1) * SPAN, cols_of(h)]
            vb = v_ref[b * SPAN : (b + 1) * SPAN, cols_of(h)]
            gram = mm_tn(kb, kb)
            pair = mm_tn(vb, kb)
            gram_s[h, b] = gram
            pair_s[h, b] = pair
            gram_sum = gram_sum + gram
            pair_sum = pair_sum + pair
        st[4 * h : 4 * h + 4] = gram_sum.reshape(4, 32, HDIM)
        st[8 + 4 * h : 12 + 4 * h] = pair_sum.reshape(4, 32, HDIM)
    exchange(st, inbox, sc1_s, sc1_r)
    take(0, 0, right)
    take(1, 2, left)
    exchanged(inbox, sc1_s, sc1_r)
    run = jnp.zeros((32, HDIM), F32)
    for i in range(CTX):
        outb[i] = run
        run = run + inbox[i]
    exchange(outb, off, sc2_s, sc2_r)
    take(0, 1, right)
    take(1, 3, left)
    exchanged(off, sc2_s, sc2_r)

    unit = eye()
    for h in range(NH):
        gram = off[4 * h : 4 * h + 4].reshape(HDIM, HDIM)
        pair = off[8 + 4 * h : 12 + 4 * h].reshape(HDIM, HDIM)
        for b in range(NB):
            p = b * NH + h
            ridged = gram + RIDGE * unit
            scale = 1.0 / jnp.sqrt(total(ridged * ridged))
            eh, el = halves(unit - scale * ridged)
            xh, xl = halves(scale * unit)
            exh[0, p] = lanes(eh, xh)
            exl[0, p] = lanes(el, xl)
            scale_s[p] = jnp.broadcast_to(scale, (8, HDIM))
            mem_h[p], mem_l[p] = halves(pair)
            gram = gram + gram_s[h, b]
            pair = pair + pair_s[h, b]

    def newton_step(j, carry):
        for p in range(NP):
            high = exh[j, p]
            low = exl[j, p]
            eh = high[:, :HDIM]
            el = low[:, :HDIM]
            new = mm(lanes(eh, el, eh), rows(high, high, low))
            iterate = high[:, HDIM:].astype(F32) + low[:, HDIM:].astype(F32) + new[:, HDIM:]
            nh, nl = halves(lanes(new[:, :HDIM], iterate))
            exh[j + 1, p] = nh
            exl[j + 1, p] = nl
        return carry

    lax.fori_loop(0, NEWTON, newton_step, 0)

    def forward(b, carry):
        for h in range(NH):
            p = b * NH + h
            qb = q_ref[rows_of(b), cols_of(h)]
            kb = k_ref[rows_of(b), cols_of(h)]
            vb = v_ref[rows_of(b), cols_of(h)]
            xh = exh[NEWTON, p][:, HDIM:]
            xl = exl[NEWTON, p][:, HDIM:]
            sh, sl = halves(mm(lanes(qb, qb), rows(xh, xl)))
            sol_h[p] = sh
            sol_l[p] = sl
            ch, cl = halves(causal(mm_nt(lanes(sh, sl), lanes(kb, kb))))
            sc_h[p] = ch
            sc_l[p] = cl
            out = mm(lanes(ch, cl), rows(vb, vb))
            mh = mem_h[p]
            out = out + mm_nt(lanes(sh, sl, sh), lanes(mh, mh, mem_l[p]))
            ho[b, :, cols_of(h)] = out.astype(BF)
        return carry

    lax.fori_loop(0, NB, forward, 0)

    def weight_cols(r, c):
        dest = lax.rem(x + r, CHIPS) * 2 + c
        return w_ref[:, pl.ds(pl.multiple_of(dest * 256, 256), 256)]

    for r in (2, 1, 3, 0):
        wcols = weight_cols(r, 1 - core)
        for b in range(NB):
            d2o[r, b] = mm(ho[b], wcols).astype(BF)
            push(d2o.at[r, b], d2i.at[r, b], d2_s.at[r, b], d2_r.at[r, b], (me, twin))

    def chip_sum(wcols, r, b):
        part = mm(ho[b], wcols)
        arrived(d2i.at[r, b], d2_s.at[r, b], d2_r.at[r, b])
        return part + d2i[r, b].astype(F32)

    wcols = weight_cols(2, core)
    for b in (0, 2, 1, 3):
        x2o[b] = chip_sum(wcols, 2, b).astype(BF)
        push(x2o.at[b], x2i.at[b], x2_s.at[b], x2_r.at[b], (me, right if b < 2 else left))
    wright = weight_cols(1, core)
    wleft = weight_cols(3, core)
    for b in (2, 3):
        xpo[b] = chip_sum(wright, 1, b).astype(BF)
        push(xpo.at[b], xli.at[b], xp_s.at[b], xp_r.at[b], (me, right))
    for b in (0, 1):
        xmo[b] = chip_sum(wleft, 3, b).astype(BF)
        push(xmo.at[b], xri.at[b], xm_s.at[b], xm_r.at[b], (me, left))
    wcols = weight_cols(0, core)
    for b in range(NB):
        loacc[b] = chip_sum(wcols, 0, b)

    for kind, b in ((0, 2), (1, 0), (0, 3), (1, 1), (2, 0), (2, 2), (2, 1), (2, 3)):
        take(kind, b)
    for b in (0, 1):
        arrived(x2i.at[b], x2_s.at[b], x2_r.at[b])
        xpo[b] = (chip_sum(wright, 1, b) + x2i[b].astype(F32)).astype(BF)
        push(xpo.at[b], xli.at[b], xp_s.at[b], xp_r.at[b], (me, right))
    for b in (2, 3):
        arrived(x2i.at[b], x2_s.at[b], x2_r.at[b])
        xmo[b] = (chip_sum(wleft, 3, b) + x2i[b].astype(F32)).astype(BF)
        push(xmo.at[b], xri.at[b], xm_s.at[b], xm_r.at[b], (me, left))
    for kind, shard in ((3, twin), (4, lax.rem(x + 3, CHIPS) * 2 + 1 - core),
                        (5, lax.rem(x + 1, CHIPS) * 2 + 1 - core),
                        (6, lax.rem(x + 2, CHIPS) * 2 + 1 - core)):
        for b in range(NB):
            arrived(ag.at[shard, b], ag_s.at[kind, b], ag_r.at[kind, b])

    for b in range(NB):
        acc = jnp.zeros((SPAN, 2 * HDIM), F32)
        for s in range(8):
            acc = acc + mm_nt(ag[s, b], w_ref[:, s * 256 : (s + 1) * 256])
        do[b] = acc.astype(BF)

    for b in range(NB):
        hot[:, b * SPAN : (b + 1) * SPAN] = ho[b].T
    for s in range(8):
        part = mm(hot[...], ag[s].reshape(NB * SPAN, 256)).astype(BF)
        wt[2 * s] = part[:, :HDIM]
        wt[2 * s + 1] = part[:, HDIM:]
    exchange(wt, gwi, gw_s, gw_r)

    def backward(b, carry):
        for h in range(NH):
            p = b * NH + h
            qb = q_ref[rows_of(b), cols_of(h)]
            kb = k_ref[rows_of(b), cols_of(h)]
            vb = v_ref[rows_of(b), cols_of(h)]
            gb = do[b, :, cols_of(h)]
            sh = sol_h[p]
            sl = sol_l[p]
            dsh, dsl = halves(causal(mm_nt(gb, vb)))
            dsolved = mm(lanes(dsh, dsl), rows(kb, kb))
            dsolved = dsolved + mm(lanes(gb, gb), rows(mem_h[p], mem_l[p]))
            dvh, dvl = halves(dsolved)
            both = mm_tn(qb, lanes(dvh, dvl))
            dinv = both[:, :HDIM] + both[:, HDIM:]
            dinv = dinv + dinv.T
            scale = scale_s[p][:1, :1]
            dh, dl = halves(-scale * dinv)
            zero = jnp.zeros((HDIM, HDIM), BF)
            dth[p] = lanes(dh, zero)
            dtl[p] = lanes(dl, zero)
            both = mm_tn(gb, lanes(sh, sl))
            dm_s[h, b] = both[:, :HDIM] + both[:, HDIM:]
            xh = exh[NEWTON, p][:, HDIM:]
            xl = exl[NEWTON, p][:, HDIM:]
            gq_ref[rows_of(b), cols_of(h)] = mm(
                lanes(dvh, dvl, dvh), rows(xh, xh, xl)
            ).astype(BF)
            both = mm_tn(dsh, lanes(sh, sl))
            dk_s[p] = both[:, :HDIM] + both[:, HDIM:] + mm_tn(dsl, sh)
            dv_s[p] = mm_tn(sc_h[p], gb) + mm_tn(sc_l[p], gb)
        return carry

    lax.fori_loop(0, NB, backward, 0)

    def dual_step(j, carry):
        for p in range(NP):
            high = exh[j, p]
            low = exl[j, p]
            dhigh = dth[p]
            dlow = dtl[p]
            first = lanes(high[:, :HDIM], dhigh[:, :HDIM])
            second = lanes(low[:, :HDIM], dlow[:, :HDIM])
            rhs = rows(dhigh, high)
            new = mm(lanes(first, second, first), rows(rhs, rhs, dlow, low))
            tangent = dhigh[:, HDIM:].astype(F32) + dlow[:, HDIM:].astype(F32) + new[:, HDIM:]
            nh, nl = halves(lanes(new[:, :HDIM], tangent))
            dth[p] = nh
            dtl[p] = nl
        return carry

    lax.fori_loop(0, NEWTON, dual_step, 0)

    for h in range(NH):
        gram_sum = jnp.zeros((HDIM, HDIM), F32)
        pair_sum = jnp.zeros((HDIM, HDIM), F32)
        for b in range(NB):
            p = b * NH + h
            value = dth[p].astype(F32) + dtl[p].astype(F32)
            trace = total(value[:, :HDIM] * unit)
            residual = exh[0, p][:, :HDIM].astype(F32) + exl[0, p][:, :HDIM].astype(F32)
            grad = value[:, HDIM:] + (trace * scale_s[p][:1, :1]) * (unit - residual)
            dg_s[h, b] = grad
            gram_sum = gram_sum + grad
            pair_sum = pair_sum + dm_s[h, b]
        st2[4 * h : 4 * h + 4] = gram_sum.reshape(4, 32, HDIM)
        st2[8 + 4 * h : 12 + 4 * h] = pair_sum.reshape(4, 32, HDIM)
    exchange(st2, inbox2, sc3_s, sc3_r)
    exchanged(inbox2, sc3_s, sc3_r)
    run = jnp.zeros((32, HDIM), F32)
    for i in reversed(range(CTX)):
        outb2[i] = run
        run = run + inbox2[i]
    exchange(outb2, off2, sc4_s, sc4_r)

    exchanged(gwi, gw_s, gw_r)
    acc = gwi[0].astype(F32)
    for i in range(1, CTX):
        acc = acc + gwi[i].astype(F32)
    gw_ref[...] = acc

    for b in range(NB):
        arrived(xli.at[b], xp_s.at[b], xp_r.at[b])
        arrived(xri.at[b], xm_s.at[b], xm_r.at[b])
        value = loacc[b] + xli[b].astype(F32) + xri[b].astype(F32)
        lo_ref[b * SPAN : (b + 1) * SPAN, :] = value.astype(BF)

    exchanged(off2, sc4_s, sc4_r)
    for h in range(NH):
        gram = off2[4 * h : 4 * h + 4].reshape(HDIM, HDIM)
        pair = off2[8 + 4 * h : 12 + 4 * h].reshape(HDIM, HDIM)
        for b in reversed(range(NB)):
            p = b * NH + h
            here = slice(b * SPAN, (b + 1) * SPAN)
            kb = k_ref[here, cols_of(h)]
            vb = v_ref[here, cols_of(h)]
            gh, gl = halves(gram)
            rh, rl = halves(pair)
            dk = dk_s[p] + mm(lanes(kb, kb), rows(gh, gl)) + mm(lanes(vb, vb), rows(rh, rl))
            gk_ref[here, cols_of(h)] = dk.astype(BF)
            dv = dv_s[p] + mm_nt(lanes(kb, kb), lanes(rh, rl))
            gv_ref[here, cols_of(h)] = dv.astype(BF)
            gram = gram + dg_s[h, b]
            pair = pair + dm_s[h, b]

    for copy in sent:
        copy.wait_send()


def shards(queries, keys, values, w_out, cotangent):
    tok = jax.ShapeDtypeStruct((NB * SPAN, NH * HDIM), BF)
    vm = lambda *shape: pltpu.VMEM(shape, BF)
    vf = lambda *shape: pltpu.VMEM(shape, F32)
    dma = lambda *shape: pltpu.SemaphoreType.DMA(shape)
    span = pl.BlockSpec(memory_space=pltpu.VMEM)
    scan = [vf(CTX, 32, HDIM)] * 4
    chunk = [vm(NB, SPAN, 256)]
    scratch = (
        [vm(8, NB, SPAN, 256)] + scan + scan
        + [vf(NH, NB, HDIM, HDIM)] * 2
        + [vm(NEWTON + 1, NP, HDIM, 256)] * 2
        + [vm(NP, HDIM, 256)] * 2
        + [vf(NP, 8, HDIM)]
        + [vm(NP, HDIM, HDIM)] * 2
        + [vm(NP, SPAN, HDIM)] * 2
        + [vm(NP, SPAN, SPAN)] * 2
        + chunk + [vm(256, NB * SPAN)] + chunk
        + [vf(NP, SPAN, HDIM)] * 2
        + [vf(NH, NB, HDIM, HDIM)] * 2
        + [vm(CHIPS, NB, SPAN, 256)] * 2
        + chunk * 6
        + [vf(NB, SPAN, 256)]
        + [vm(CTX, 256, HDIM)] * 2
        + [dma(7, NB)] * 2
        + [dma(CTX - 1)] * 10
        + [dma(CHIPS, NB)] * 2
        + [dma(NB)] * 6
    )
    return pl.pallas_call(
        kernel,
        out_shape=(tok, tok, tok, tok, jax.ShapeDtypeStruct((256, HDIM), F32)),
        in_specs=[span] * 5,
        out_specs=[span] * 5,
        scratch_shapes=scratch,
        compiler_params=pltpu.CompilerParams(
            collective_id=0, has_side_effects=True, vmem_limit_bytes=60 * 1024 * 1024
        ),
        name="mesa_layer",
    )(queries, keys, values, w_out, cotangent)


def solution(mesh):
    placed = (P("ctx", "head"), P("ctx", "head"), P("ctx", "head"), P("head", None), P("ctx", "head"))
    return jax.shard_map(
        shards,
        mesh=mesh,
        in_specs=placed,
        out_specs=(P("ctx", "head"), P("ctx", "head"), P("ctx", "head"), P("ctx", "head"), P("head", "ctx")),
        check_vma=False,
    )
```

```python
import jax
import jax.numpy as jnp
from jax import lax
from jax.experimental import pallas as pl
from jax.experimental.pallas import tpu as pltpu
from jax.sharding import PartitionSpec as P

HDIM = 128
SPAN = 256
NEWTON = 8
RIDGE = 1.0
NB = 4
NH = 2
NP = NB * NH
CTX = 16
CHIPS = 4
VMEM_LIMIT = 103 * 512 * 1024
F32 = jnp.float32
BF = jnp.bfloat16
MESH = pl.DeviceIdType.MESH


def mm(a, b):
    return lax.dot_general(a, b, (((1,), (0,)), ((), ())), preferred_element_type=F32)


def mm_nt(a, b):
    return lax.dot_general(a, b, (((1,), (1,)), ((), ())), preferred_element_type=F32)


def mm_tn(a, b):
    return lax.dot_general(a, b, (((0,), (0,)), ((), ())), preferred_element_type=F32)


def rows(*parts):
    return jnp.concatenate(parts, axis=0)


def lanes(*parts):
    return jnp.concatenate(parts, axis=1)


def halves(value):
    high = value.astype(BF)
    return high, (value - high.astype(F32)).astype(BF)


def total(value):
    return jnp.sum(jnp.sum(value, axis=1, keepdims=True), axis=0, keepdims=True)


def eye():
    shape = (HDIM, HDIM)
    return (
        lax.broadcasted_iota(jnp.int32, shape, 0) == lax.broadcasted_iota(jnp.int32, shape, 1)
    ).astype(F32)


def high_low(high, low, p):
    return high[0, p][:, :HDIM].astype(F32) + low[0, p][:, :HDIM].astype(F32)


def causal(value):
    shape = (SPAN, SPAN)
    keep = lax.broadcasted_iota(jnp.int32, shape, 0) >= lax.broadcasted_iota(jnp.int32, shape, 1)
    return jnp.where(keep, value, 0.0)


def kernel(
    q_hbm, k_hbm, v_hbm, w_hbm, cot_hbm,
    lo_ref, gq_ref, gk_ref, gv_ref, gw_ref,
    q_ref, k_ref, v_ref, w_ref, cot_ref,
    ag, st, inbox, outb, off, st2, inbox2, outb2, off2,
    gram_s, pair_s, exh, exl, dt, tan_s, scale_s, mem_h, mem_l, memt_h, memt_l,
    sol_h, sol_l, sc, ds, dv, ho, hot, dacc, do, dg_s, dm_s,
    d2o, d2i, own, x2o, x2i, xpo, xmo, xli, xri, wa, wb, ga, gb, sa, sb, ra, rb,
    in_s, ag_s, ag_r, sc1_s, sc1_r, sc2_s, sc2_r, sc3_s, sc3_r, sc4_s, sc4_r,
    gw1_s, gw1_r, gw2_s, gw2_r, d2_s, d2_r, x2_s, x2_r, xp_s, xp_r, xm_s, xm_r,
):
    me = lax.axis_index("ctx")
    hd = lax.axis_index("head")
    x = lax.div(hd, 2)
    y = lax.div(me, 4)
    z = lax.rem(me, 4)
    core = lax.rem(hd, 2)
    right = lax.rem(x + 1, CHIPS) * 2 + core
    left = lax.rem(x + 3, CHIPS) * 2 + core
    far = lax.rem(x + 2, CHIPS) * 2 + core
    twin = x * 2 + 1 - core
    other = (left + 1 - 2 * core, right + 1 - 2 * core, far + 1 - 2 * core)
    sent = []
    scope = []

    def mark(name=None):
        if scope:
            scope.pop().__exit__(None, None, None)
        if name is not None:
            now = jax.named_scope(name)
            now.__enter__()
            scope.append(now)

    def remote(src, dst, ss, rs, dev):
        return pltpu.make_async_remote_copy(
            src_ref=src, dst_ref=dst, send_sem=ss, recv_sem=rs, device_id=dev, device_id_type=MESH
        )

    def push(src, dst, ss, rs, dev):
        copy = remote(src, dst, ss, rs, dev)
        copy.start()
        sent.append(copy)

    def arrived(dst, ss, rs):
        remote(dst, dst, ss, rs, (me, twin)).wait_recv()

    def exchange(src, dst, ss, rs):
        for d in range(1, CTX):
            peer = lax.rem(me + d, CTX)
            push(src.at[peer], dst.at[me], ss.at[d - 1], rs.at[d - 1], (peer, hd))

    def exchanged(dst, ss, rs):
        for d in range(1, CTX):
            peer = lax.rem(me + CTX - d, CTX)
            arrived(dst.at[peer], ss.at[d - 1], rs.at[d - 1])

    def rows_of(b):
        return slice(b * SPAN, (b + 1) * SPAN)

    def cols_of(h):
        return slice(h * HDIM, (h + 1) * HDIM)

    mark("entry")
    barrier = pltpu.get_barrier_semaphore()
    for d in range(1, CTX):
        pl.semaphore_signal(barrier, inc=1, device_id=(lax.rem(me + d, CTX), hd), device_id_type=MESH)
    for dev in (right, left, twin):
        pl.semaphore_signal(barrier, inc=1, device_id=(me, dev), device_id_type=MESH)
    loads = [
        pltpu.make_async_copy(src, dst, in_s.at[i])
        for i, (src, dst) in enumerate(
            ((k_hbm, k_ref), (v_hbm, v_ref), (cot_hbm, cot_ref), (q_hbm, q_ref), (w_hbm, w_ref))
        )
    ]
    for load in loads:
        load.start()

    loads[0].wait()
    loads[1].wait()
    mark("gram")
    for h in range(NH):
        gram_sum = jnp.zeros((HDIM, HDIM), F32)
        pair_sum = jnp.zeros((HDIM, HDIM), F32)
        for b in range(NB):
            kb = k_ref[rows_of(b), cols_of(h)]
            vb = v_ref[rows_of(b), cols_of(h)]
            gram = mm_tn(kb, kb)
            pair = mm_tn(vb, kb)
            gram_s[h, b] = gram
            pair_s[h, b] = pair
            gram_sum = gram_sum + gram
            pair_sum = pair_sum + pair
        st[4 * h : 4 * h + 4] = gram_sum.reshape(4, 32, HDIM)
        st[8 + 4 * h : 12 + 4 * h] = pair_sum.reshape(4, 32, HDIM)
    inbox[me] = st[me]
    loads[2].wait()
    mark("barrier")
    pl.semaphore_wait(barrier, CTX - 1 + 3)

    exchange(st, inbox, sc1_s, sc1_r)
    for b in range(NB):
        for kind, dev, blk in ((0, right, b), (1, left, (b + 2) % NB)):
            push(
                cot_ref.at[pl.ds(blk * SPAN, SPAN), :], ag.at[hd, blk],
                ag_s.at[kind, blk], ag_r.at[kind, blk], (me, dev),
            )
    for b in range(NB):
        push(
            cot_ref.at[pl.ds(b * SPAN, SPAN), :], ag.at[hd, b],
            ag_s.at[3, b], ag_r.at[3, b], (me, twin),
        )
        ag[hd, b] = cot_ref[rows_of(b), :]

    def take(kind, b, relay=None):
        shard = (left, right, far)[kind]
        here = ag.at[shard, b]
        arrived(here, ag_s.at[kind, b], ag_r.at[kind, b])
        if relay is not None:
            push(here, here, ag_s.at[2, b], ag_r.at[2, b], (me, relay))
        push(here, here, ag_s.at[4 + kind, b], ag_r.at[4 + kind, b], (me, twin))

    def scan(box, out, order):
        run = jnp.zeros((32, HDIM), F32)
        for i in order:
            out[i] = run.astype(out.dtype)
            run = run + box[i].astype(F32)

    def twin_took(kind, blocks=range(NB)):
        shard = twin if kind == 3 else other[kind - 4]
        for b in blocks:
            arrived(ag.at[shard, b], ag_s.at[kind, b], ag_r.at[kind, b])

    def grad_heads(ids, start=False):
        for b in range(NB):
            acc = None if start else dacc[rows_of(b), :]
            for s in ids:
                cols = pl.ds(pl.multiple_of(s * 256, 256), 256)
                part = mm_nt(ag[s, b], w_ref[:, cols])
                acc = part if acc is None else acc + part
            dacc[rows_of(b), :] = acc

    unit = eye()
    loads[3].wait()
    loads[4].wait()
    mark("scan1w")
    exchanged(inbox, sc1_s, sc1_r)
    mark("scan2s")
    scan(inbox, outb, range(CTX))
    exchange(outb, off, sc2_s, sc2_r)
    off[me] = outb[me]
    mark("relay")
    take(0, 0, right)
    take(1, 2, left)
    take(0, 1, right)
    take(1, 3, left)
    twin_took(3)
    mark("do1")
    grad_heads((hd, twin), True)
    mark("scan2w")
    exchanged(off, sc2_s, sc2_r)

    mark("newton")
    for h in range(NH):
        gram = off[4 * h : 4 * h + 4].reshape(HDIM, HDIM)
        pair = off[8 + 4 * h : 12 + 4 * h].reshape(HDIM, HDIM)
        for b in range(NB):
            p = b * NH + h
            ridged = gram + RIDGE * unit
            scale = 1.0 / jnp.sqrt(total(ridged * ridged))
            eh, el = halves(unit - scale * ridged)
            xh, xl = halves(scale * unit)
            exh[0, p] = lanes(eh, xh)
            exl[0, p] = lanes(el, xl)
            scale_s[p] = jnp.broadcast_to(scale, (8, HDIM))
            mem_h[p], mem_l[p] = halves(pair)
            memt_h[p], memt_l[p] = halves(pair.T)
            gram = gram + gram_s[h, b]
            pair = pair + pair_s[h, b]

    for j in range(NEWTON):
        for p in range(NP):
            high = exh[j, p]
            low = exl[j, p]
            eh = high[:, :HDIM]
            el = low[:, :HDIM]
            new = mm(lanes(eh, el, eh), rows(high, high, low))
            iterate = high[:, HDIM:].astype(F32) + low[:, HDIM:].astype(F32) + new[:, HDIM:]
            nh, nl = halves(lanes(new[:, :HDIM], iterate))
            exh[j + 1, p] = nh
            exl[j + 1, p] = nl

    mark("take1")
    for kind, b in ((0, 2), (1, 0), (0, 3), (1, 1)):
        take(kind, b)
    mark("forward")
    for p in range(NP):
        b, h = divmod(p, NH)
        qb = q_ref[rows_of(b), cols_of(h)]
        kb = k_ref[rows_of(b), cols_of(h)]
        vb = v_ref[rows_of(b), cols_of(h)]
        xh = exh[NEWTON, p][:, HDIM:]
        xl = exl[NEWTON, p][:, HDIM:]
        sh, sl = halves(mm(lanes(qb, qb), rows(xh, xl)))
        sol_h[p] = sh
        sol_l[p] = sl
        ch = causal(mm_nt(lanes(sh, sl), lanes(kb, kb))).astype(BF)
        sc[p] = ch
        out = mm(lanes(ch, sh, sh), rows(vb, memt_h[p], memt_l[p]))
        ho[rows_of(b), cols_of(h)] = out.astype(BF)

    def partial(r, c):
        dest = lax.rem(x + r, CHIPS) * 2 + c
        return mm(ho[...], w_ref[:, pl.ds(pl.multiple_of(dest * 256, 256), 256)])

    def to_twin(r):
        d2o[r] = partial(r, 1 - core).astype(BF)

    def send_twin(r):
        push(d2o.at[r], d2i.at[r], d2_s.at[r], d2_r.at[r], (me, twin))

    def from_twin(r):
        arrived(d2i.at[r], d2_s.at[r], d2_r.at[r])

    def chip_sum(r, b):
        return own[r, rows_of(b), :] + d2i[r, rows_of(b), :].astype(F32)

    mark("take2")
    for kind, b in ((2, 0), (2, 2)):
        take(kind, b)
    mark("rs1")
    to_twin(2)
    send_twin(2)
    to_twin(1)
    to_twin(3)
    send_twin(1)
    send_twin(3)
    own[2] = partial(2, core)
    mark("rs2")
    from_twin(2)
    for b in range(NB):
        x2o[b] = chip_sum(2, b).astype(BF)
    for b in (0, 2, 1, 3):
        push(x2o.at[b], x2i.at[b], x2_s.at[b], x2_r.at[b], (me, right if b < 2 else left))
    own[1] = partial(1, core)
    own[3] = partial(3, core)
    to_twin(0)
    own[0] = partial(0, core)
    send_twin(0)
    from_twin(1)
    from_twin(3)
    for b in (2, 3):
        xpo[b] = chip_sum(1, b).astype(BF)
        xmo[3 - b] = chip_sum(3, 3 - b).astype(BF)
    for b in (2, 3):
        push(xpo.at[b], xli.at[b], xp_s.at[b], xp_r.at[b], (me, right))
        push(xmo.at[3 - b], xri.at[3 - b], xm_s.at[3 - b], xm_r.at[3 - b], (me, left))

    mark("take3")
    for kind, b in ((2, 1), (2, 3)):
        take(kind, b)
    twin_took(4)
    twin_took(5)
    mark("do2")
    grad_heads((left, right, other[0], other[1]))
    mark("agtwin")
    twin_took(6)
    mark("do3")
    grad_heads((far, other[2]))
    do[...] = dacc[...].astype(BF)

    mark("gwpart")
    for b in range(NB):
        hot[:, rows_of(b)] = ho[rows_of(b), :].T
    for s in range(8):
        part = mm(hot[...], ag[s].reshape(NB * SPAN, 256)).astype(BF)
        for i in range(2):
            dy, dz = divmod(2 * s + i, 4)
            wa[dz, dy] = part[:HDIM, cols_of(i)]
            wb[dy, dz] = part[HDIM:, cols_of(i)]

    def along_z(d):
        return y * 4 + lax.rem(z + d, 4)

    def along_y(d):
        return lax.rem(y + d, 4) * 4 + z

    def round_send(src_a, dst_a, src_b, dst_b, ss, rs, swap):
        to_a, to_b = (along_y, along_z) if swap else (along_z, along_y)
        at_a, at_b = (y, z) if swap else (z, y)
        for d in range(1, 4):
            push(src_a.at[lax.rem(at_a + d, 4)], dst_a.at[at_a], ss.at[d - 1], rs.at[d - 1], (to_a(d), hd))
            push(src_b.at[lax.rem(at_b + d, 4)], dst_b.at[at_b], ss.at[d + 2], rs.at[d + 2], (to_b(d), hd))

    def round_wait(dst_a, dst_b, ss, rs, swap):
        at_a, at_b = (y, z) if swap else (z, y)
        for d in range(1, 4):
            arrived(dst_a.at[lax.rem(at_a + 4 - d, 4)], ss.at[d - 1], rs.at[d - 1])
            arrived(dst_b.at[lax.rem(at_b + 4 - d, 4)], ss.at[d + 2], rs.at[d + 2])

    def four(ref):
        return (ref[0].astype(F32) + ref[1].astype(F32)) + (ref[2].astype(F32) + ref[3].astype(F32))

    round_send(wa, ga, wb, gb, gw1_s, gw1_r, False)
    ga[z] = wa[z]
    gb[y] = wb[y]

    mark("bwd1")
    for p in range(NP):
        b, h = divmod(p, NH)
        qb = q_ref[rows_of(b), cols_of(h)]
        kb = k_ref[rows_of(b), cols_of(h)]
        vb = v_ref[rows_of(b), cols_of(h)]
        dob = do[rows_of(b), cols_of(h)]
        dsh = causal(mm_nt(dob, vb)).astype(BF)
        ds[p] = dsh
        dsolved = mm(lanes(dsh, dob, dob), rows(kb, mem_h[p], mem_l[p])).astype(BF)
        dv[p] = dsolved
        dinv = mm_tn(qb, dsolved)
        dinv = -scale_s[p][:1, :1] * (dinv + dinv.T)
        dt[0, p] = lanes(dinv.astype(BF), jnp.zeros((HDIM, HDIM), BF))
        tan_s[p] = jnp.zeros((HDIM, HDIM), F32)
        both = mm_tn(dob, lanes(sol_h[p], sol_l[p]))
        dm_s[h, b] = both[:, :HDIM] + both[:, HDIM:]

    mark("dual")
    for j in range(NEWTON):
        for p in range(NP):
            high = exh[j, p]
            here = dt[j % 2, p]
            new = mm(lanes(high[:, :HDIM], here[:, :HDIM]), rows(here, high))
            tangent = tan_s[p] + new[:, HDIM:]
            tan_s[p] = tangent
            if j < NEWTON - 1:
                dt[(j + 1) % 2, p] = lanes(new[:, :HDIM].astype(BF), tangent.astype(BF))
            else:
                b, h = divmod(p, NH)
                trace = total(new[:, :HDIM] * unit)
                residual = high_low(exh, exl, p)
                dg_s[h, b] = tangent + (trace * scale_s[p][:1, :1]) * (unit - residual)

    for h in range(NH):
        gram_sum = (dg_s[h, 0] + dg_s[h, 1]) + (dg_s[h, 2] + dg_s[h, 3])
        pair_sum = (dm_s[h, 0] + dm_s[h, 1]) + (dm_s[h, 2] + dm_s[h, 3])
        st2[4 * h : 4 * h + 4] = gram_sum.reshape(4, 32, HDIM).astype(BF)
        st2[8 + 4 * h : 12 + 4 * h] = pair_sum.reshape(4, 32, HDIM).astype(BF)
    exchange(st2, inbox2, sc3_s, sc3_r)
    inbox2[me] = st2[me]

    mark("bwd2")
    for p in range(NP):
        b, h = divmod(p, NH)
        dob = do[rows_of(b), cols_of(h)]
        xs = rows(exh[NEWTON, p][:, HDIM:], exl[NEWTON, p][:, HDIM:])
        gq_ref[rows_of(b), cols_of(h)] = mm(lanes(dv[p], dv[p]), xs).astype(BF)
        both = mm_tn(ds[p], lanes(sol_h[p], sol_l[p]))
        own[2, rows_of(b), cols_of(h)] = both[:, :HDIM] + both[:, HDIM:]
        dacc[rows_of(b), cols_of(h)] = mm_tn(sc[p], dob)

    mark("gw2")
    round_wait(ga, gb, gw1_s, gw1_r, False)
    for i in range(4):
        sa[i] = ((ga[0, i].astype(F32) + ga[1, i].astype(F32)) + (ga[2, i].astype(F32) + ga[3, i].astype(F32))).astype(BF)
        sb[i] = ((gb[0, i].astype(F32) + gb[1, i].astype(F32)) + (gb[2, i].astype(F32) + gb[3, i].astype(F32))).astype(BF)
    round_send(sa, ra, sb, rb, gw2_s, gw2_r, True)
    ra[y] = sa[y]
    rb[z] = sb[z]

    mark("rs3")
    for b in range(NB):
        arrived(x2i.at[b], x2_s.at[b], x2_r.at[b])
    for b in (0, 1):
        xpo[b] = (chip_sum(1, b) + x2i[b].astype(F32)).astype(BF)
        xmo[3 - b] = (chip_sum(3, 3 - b) + x2i[3 - b].astype(F32)).astype(BF)
    for b in (0, 1):
        push(xpo.at[b], xli.at[b], xp_s.at[b], xp_r.at[b], (me, right))
        push(xmo.at[3 - b], xri.at[3 - b], xm_s.at[3 - b], xm_r.at[3 - b], (me, left))

    mark("scan3w")
    exchanged(inbox2, sc3_s, sc3_r)
    mark("scan4s")
    scan(inbox2, outb2, reversed(range(CTX)))
    exchange(outb2, off2, sc4_s, sc4_r)
    off2[me] = outb2[me]
    from_twin(0)

    mark("gw3")
    round_wait(ra, rb, gw2_s, gw2_r, True)
    gw_ref[:HDIM, :] = four(ra)
    gw_ref[HDIM:, :] = four(rb)

    mark("scan4w")
    exchanged(off2, sc4_s, sc4_r)
    mark("final")
    for h in range(NH):
        gram = off2[4 * h : 4 * h + 4].reshape(HDIM, HDIM).astype(F32)
        pair = off2[8 + 4 * h : 12 + 4 * h].reshape(HDIM, HDIM).astype(F32)
        for b in reversed(range(NB)):
            here = rows_of(b)
            kb = k_ref[here, cols_of(h)]
            vb = v_ref[here, cols_of(h)]
            rh = pair.astype(BF)
            dk = own[2, here, cols_of(h)] + mm(lanes(kb, vb), rows(gram.astype(BF), rh))
            gk_ref[here, cols_of(h)] = dk.astype(BF)
            gv_ref[here, cols_of(h)] = (dacc[here, cols_of(h)] + mm_nt(kb, rh)).astype(BF)
            gram = gram + dg_s[h, b]
            pair = pair + dm_s[h, b]

    mark("lofin")
    for b in range(NB):
        arrived(xli.at[b], xp_s.at[b], xp_r.at[b])
        arrived(xri.at[b], xm_s.at[b], xm_r.at[b])
    for b in range(NB):
        value = chip_sum(0, b) + xli[b].astype(F32) + xri[b].astype(F32)
        lo_ref[rows_of(b), :] = value.astype(BF)

    mark("waitsend")
    for copy in sent:
        copy.wait_send()
    mark()


def write_out(*refs):
    sources, targets, sems = refs[:5], refs[5:10], refs[10]
    copies = [
        pltpu.make_async_copy(src, dst, sems.at[i])
        for i, (src, dst) in enumerate(zip(sources, targets))
    ]
    for copy in copies:
        copy.start()
    for copy in copies:
        copy.wait()


def shards(queries, keys, values, w_out, cotangent):
    tok = jax.ShapeDtypeStruct((NB * SPAN, NH * HDIM), BF)
    shapes = (tok, tok, tok, tok, jax.ShapeDtypeStruct((256, HDIM), F32))
    vm = lambda *shape: pltpu.VMEM(shape, BF)
    vf = lambda *shape: pltpu.VMEM(shape, F32)
    dma = lambda *shape: pltpu.SemaphoreType.DMA(shape)
    span = pl.BlockSpec(memory_space=pltpu.VMEM)
    anywhere = pl.BlockSpec(memory_space=pl.ANY)
    chunk = [vm(NB, SPAN, 256)]
    flat = [vm(NB * SPAN, 256)]
    scratch = (
        flat * 3 + [vm(256, 2048)] + flat
        + [vm(8, NB, SPAN, 256)]
        + [vf(CTX, 32, HDIM)] * 4 + [vm(CTX, 32, HDIM)] * 4
        + [vf(NH, NB, HDIM, HDIM)] * 2
        + [vm(NEWTON + 1, NP, HDIM, 256)] * 2
        + [vm(2, NP, HDIM, 256), vf(NP, HDIM, HDIM)]
        + [vf(NP, 8, HDIM)]
        + [vm(NP, HDIM, HDIM)] * 4
        + [vm(NP, SPAN, HDIM)] * 2
        + [vm(NP, SPAN, SPAN)] * 2
        + [vm(NP, SPAN, HDIM)]
        + flat + [vm(256, NB * SPAN), vf(NB * SPAN, 256)] + flat
        + [vf(NH, NB, HDIM, HDIM)] * 2
        + [vm(CHIPS, NB * SPAN, 256)] * 2
        + [vf(CHIPS, NB * SPAN, 256)]
        + chunk * 6
        + [vm(4, 4, HDIM, HDIM)] * 4
        + [vm(4, HDIM, HDIM)] * 4
        + [dma(5)]
        + [dma(7, NB)] * 2
        + [dma(CTX - 1)] * 8
        + [dma(6)] * 4
        + [dma(CHIPS)] * 2
        + [dma(NB)] * 6
    )
    results = pl.pallas_call(
        kernel,
        out_shape=shapes,
        in_specs=[pl.BlockSpec(memory_space=pltpu.HBM)] * 5,
        out_specs=[span] * 5,
        scratch_shapes=scratch,
        compiler_params=pltpu.CompilerParams(
            collective_id=0, has_side_effects=True, vmem_limit_bytes=VMEM_LIMIT
        ),
        name="mesa_layer",
    )(queries, keys, values, w_out, cotangent)
    return pl.pallas_call(
        write_out,
        out_shape=shapes,
        in_specs=[span] * 5,
        out_specs=[anywhere] * 5,
        scratch_shapes=[dma(5)],
        compiler_params=pltpu.CompilerParams(vmem_limit_bytes=1 * 1024 * 1024),
        name="write_out",
    )(*results)


def solution(mesh):
    placed = (P("ctx", "head"), P("ctx", "head"), P("ctx", "head"), P("head", None), P("ctx", "head"))
    return jax.shard_map(
        shards,
        mesh=mesh,
        in_specs=placed,
        out_specs=(P("ctx", "head"), P("ctx", "head"), P("ctx", "head"), P("ctx", "head"), P("head", "ctx")),
        check_vma=False,
    )
```

```python
import jax
import jax.numpy as jnp
from jax import lax
from jax.experimental import pallas as pl
from jax.experimental.pallas import tpu as pltpu
from jax.sharding import PartitionSpec as P

HDIM = 128
SPAN = 256
NEWTON = 8
RIDGE = 1.0
NB = 4
NH = 2
NP = NB * NH
CTX = 16
CHIPS = 4
VMEM_LIMIT = 103 * 512 * 1024
F32 = jnp.float32
BF = jnp.bfloat16
MESH = pl.DeviceIdType.MESH


def mm(a, b):
    return lax.dot_general(a, b, (((1,), (0,)), ((), ())), preferred_element_type=F32)


def mm_nt(a, b):
    return lax.dot_general(a, b, (((1,), (1,)), ((), ())), preferred_element_type=F32)


def mm_tn(a, b):
    return lax.dot_general(a, b, (((0,), (0,)), ((), ())), preferred_element_type=F32)


def rows(*parts):
    return jnp.concatenate(parts, axis=0)


def lanes(*parts):
    return jnp.concatenate(parts, axis=1)


def halves(value):
    high = value.astype(BF)
    return high, (value - high.astype(F32)).astype(BF)


def total(value):
    return jnp.sum(jnp.sum(value, axis=1, keepdims=True), axis=0, keepdims=True)


def eye():
    shape = (HDIM, HDIM)
    return (
        lax.broadcasted_iota(jnp.int32, shape, 0) == lax.broadcasted_iota(jnp.int32, shape, 1)
    ).astype(F32)


def high_low(high, low, p):
    return high[0, p][:, :HDIM].astype(F32) + low[0, p][:, :HDIM].astype(F32)


def causal(value):
    shape = (SPAN, SPAN)
    keep = lax.broadcasted_iota(jnp.int32, shape, 0) >= lax.broadcasted_iota(jnp.int32, shape, 1)
    return jnp.where(keep, value, 0.0)


def kernel(
    q_hbm, k_hbm, v_hbm, w_hbm, cot_hbm,
    lo_ref, gq_ref, gk_ref, gv_ref, gw_ref,
    q_ref, k_ref, v_ref, w_ref, cot_ref,
    ag, st, inbox, outb, off, st2, inbox2, outb2, off2,
    pt, pinbox, poutb, poff, pt2, pinbox2, poutb2, poff2,
    gram_s, pair_s, exh, exl, dt, tan_s, scale_s, mem_h, mem_l, memt_h, memt_l,
    sol_h, sol_l, sc, ds, dv, ho, hot, dacc, do, dg_s, dm_s,
    d2o, d2i, own, x2o, x2i, xpo, xmo, xli, xri, wa, wb, ga, gb, sa, sb, ra, rb,
    in_s, send_s, ex_r, near_r, twin_r, gw_r, d2_r, far_r,
):
    me = lax.axis_index("ctx")
    hd = lax.axis_index("head")
    x = lax.div(hd, 2)
    y = lax.div(me, 4)
    z = lax.rem(me, 4)
    core = lax.rem(hd, 2)
    right = lax.rem(x + 1, CHIPS) * 2 + core
    left = lax.rem(x + 3, CHIPS) * 2 + core
    far = lax.rem(x + 2, CHIPS) * 2 + core
    twin = x * 2 + 1 - core
    other = (left + 1 - 2 * core, right + 1 - 2 * core, far + 1 - 2 * core)
    scope = []

    def mark(name=None):
        if scope:
            scope.pop().__exit__(None, None, None)
        if name is not None:
            now = jax.named_scope(name)
            now.__enter__()
            scope.append(now)

    def remote(src, dst, ss, rs, dev):
        return pltpu.make_async_remote_copy(
            src_ref=src, dst_ref=dst, send_sem=ss, recv_sem=rs, device_id=dev, device_id_type=MESH
        )

    def push(src, dst, ss, rs, dev):
        remote(src, dst, ss, rs, dev).start()

    def arrived(dst, rs):
        remote(dst, dst, send_s.at[0], rs, (me, twin)).wait_recv()

    def left_here(src, ss):
        remote(src, src, ss, ex_r.at[0], (me, twin)).wait_send()

    def exchange(src, dst, i):
        for d in range(1, CTX):
            peer = lax.rem(me + d, CTX)
            push(src.at[peer], dst.at[me], send_s.at[i], ex_r.at[i], (peer, hd))

    def exchanged(dst, i):
        arrived(dst.at[pl.ds(0, CTX - 1)], ex_r.at[i])

    def rows_of(b):
        return slice(b * SPAN, (b + 1) * SPAN)

    def cols_of(h):
        return slice(h * HDIM, (h + 1) * HDIM)

    mark("entry")
    barrier = pltpu.get_barrier_semaphore()
    for d in range(1, CTX):
        pl.semaphore_signal(barrier, inc=1, device_id=(lax.rem(me + d, CTX), hd), device_id_type=MESH)
    for dev in (right, left, twin):
        pl.semaphore_signal(barrier, inc=1, device_id=(me, dev), device_id_type=MESH)
    loads = [
        pltpu.make_async_copy(src, dst, in_s.at[i])
        for i, (src, dst) in enumerate(
            ((k_hbm, k_ref), (v_hbm, v_ref), (cot_hbm, cot_ref), (q_hbm, q_ref), (w_hbm, w_ref))
        )
    ]
    for load in loads[:3]:
        load.start()

    loads[0].wait()
    loads[1].wait()
    for load in loads[3:]:
        load.start()
    mark("gram")
    for h in range(NH):
        gram_sum = jnp.zeros((HDIM, HDIM), F32)
        pair_sum = jnp.zeros((HDIM, HDIM), F32)
        for b in range(NB):
            kb = k_ref[rows_of(b), cols_of(h)]
            vb = v_ref[rows_of(b), cols_of(h)]
            gram = mm_tn(kb, kb)
            pair = mm_tn(vb, kb)
            gram_s[h, b] = gram
            pair_s[h, b] = pair
            gram_sum = gram_sum + gram
            pair_sum = pair_sum + pair
        st[8 * h : 8 * h + 8] = gram_sum.reshape(8, 16, HDIM)
        pt[8 * h : 8 * h + 8] = pair_sum.reshape(8, 16, HDIM)
    inbox[me] = st[me]
    pinbox[me] = pt[me]
    loads[2].wait()
    mark("barrier")
    pl.semaphore_wait(barrier, CTX - 1 + 3)

    exchange(st, inbox, 0)
    for b in range(NB):
        for kind, dev, blk in ((0, right, b), (1, left, (b + 2) % NB)):
            push(
                cot_ref.at[pl.ds(blk * SPAN, SPAN), :], ag.at[hd, blk],
                send_s.at[8], near_r.at[kind, blk], (me, dev),
            )
    for b in range(NB):
        push(
            cot_ref.at[pl.ds(b * SPAN, SPAN), :], ag.at[hd, b],
            send_s.at[8], twin_r.at[0], (me, twin),
        )
        ag[hd, b] = cot_ref[rows_of(b), :]
    exchange(pt, pinbox, 4)

    def take(kind, b, relay=None):
        shard = (left, right, far)[kind]
        here = ag.at[shard, b]
        arrived(here, near_r.at[kind, b])
        if relay is not None:
            push(here, here, send_s.at[8], near_r.at[2, b], (me, relay))
        push(here, here, send_s.at[8], twin_r.at[1 + kind], (me, twin))

    def scan(box, out, order):
        run = jnp.zeros((16, HDIM), F32)
        for i in order:
            out[i] = run.astype(out.dtype)
            run = run + box[i].astype(F32)

    def twin_took(kind):
        arrived(ag.at[(twin, *other)[kind]], twin_r.at[kind])

    def grad_heads(ids, start=False):
        for b in range(NB):
            acc = None if start else dacc[rows_of(b), :]
            for s in ids:
                cols = pl.ds(pl.multiple_of(s * 256, 256), 256)
                part = mm_nt(ag[s, b], w_ref[:, cols])
                acc = part if acc is None else acc + part
            dacc[rows_of(b), :] = acc

    unit = eye()
    loads[3].wait()
    loads[4].wait()
    mark("scan1w")
    exchanged(inbox, 0)
    mark("scan2s")
    scan(inbox, outb, range(CTX))
    exchange(outb, off, 1)
    off[me] = outb[me]
    exchanged(pinbox, 4)
    scan(pinbox, poutb, range(CTX))
    exchange(poutb, poff, 5)
    poff[me] = poutb[me]
    mark("relay")
    take(0, 0, right)
    take(1, 2, left)
    twin_took(0)
    mark("do1")
    grad_heads((hd, twin), True)
    mark("scan2w")
    exchanged(off, 1)

    mark("newton")
    for h in range(NH):
        gram = off[8 * h : 8 * h + 8].reshape(HDIM, HDIM)
        for b in range(NB):
            p = b * NH + h
            ridged = gram + RIDGE * unit
            scale = 1.0 / jnp.sqrt(total(ridged * ridged))
            eh, el = halves(unit - scale * ridged)
            xh, xl = halves(scale * unit)
            exh[0, p] = lanes(eh, xh)
            exl[0, p] = lanes(el, xl)
            scale_s[p] = jnp.broadcast_to(scale, (8, HDIM))
            gram = gram + gram_s[h, b]

    for j in range(NEWTON):
        if j == 3:
            take(0, 1, right)
            take(1, 3, left)
        for p in range(NP):
            high = exh[j, p]
            low = exl[j, p]
            eh = high[:, :HDIM]
            el = low[:, :HDIM]
            new = mm(lanes(eh, el, eh), rows(high, high, low))
            iterate = high[:, HDIM:].astype(F32) + low[:, HDIM:].astype(F32) + new[:, HDIM:]
            nh, nl = halves(lanes(new[:, :HDIM], iterate))
            exh[j + 1, p] = nh
            exl[j + 1, p] = nl

    mark("pair")
    exchanged(poff, 5)
    for h in range(NH):
        pair = poff[8 * h : 8 * h + 8].reshape(HDIM, HDIM)
        for b in range(NB):
            p = b * NH + h
            mem_h[p], mem_l[p] = halves(pair)
            memt_h[p], memt_l[p] = halves(pair.T)
            pair = pair + pair_s[h, b]

    mark("forward")
    for p in range(NP):
        b, h = divmod(p, NH)
        qb = q_ref[rows_of(b), cols_of(h)]
        kb = k_ref[rows_of(b), cols_of(h)]
        vb = v_ref[rows_of(b), cols_of(h)]
        xh = exh[NEWTON, p][:, HDIM:]
        xl = exl[NEWTON, p][:, HDIM:]
        sh, sl = halves(mm(lanes(qb, qb), rows(xh, xl)))
        sol_h[p] = sh
        sol_l[p] = sl
        ch = causal(mm_nt(lanes(sh, sl), lanes(kb, kb))).astype(BF)
        sc[p] = ch
        out = mm(lanes(ch, sh, sh), rows(vb, memt_h[p], memt_l[p]))
        ho[rows_of(b), cols_of(h)] = out.astype(BF)

    def partial(r, c):
        dest = lax.rem(x + r, CHIPS) * 2 + c
        return mm(ho[...], w_ref[:, pl.ds(pl.multiple_of(dest * 256, 256), 256)])

    def to_twin(r):
        d2o[r] = partial(r, 1 - core).astype(BF)

    def send_twin(r):
        push(d2o.at[r], d2i.at[r], send_s.at[9], d2_r.at[r], (me, twin))

    def from_twin(r):
        arrived(d2i.at[r], d2_r.at[r])

    def chip_sum(r, b):
        return own[r, rows_of(b), :] + d2i[r, rows_of(b), :].astype(F32)

    mark("take2")
    for kind, b in ((0, 2), (1, 0), (0, 3), (1, 1)):
        take(kind, b)
    mark("rs1")
    to_twin(2)
    send_twin(2)
    own[2] = partial(2, core)
    to_twin(1)
    to_twin(3)
    send_twin(1)
    send_twin(3)
    mark("rs2b")
    own[1] = partial(1, core)
    own[3] = partial(3, core)
    mark("take2b")
    for kind, b in ((2, 0), (2, 2)):
        take(kind, b)
    mark("take4")
    twin_took(1)
    twin_took(2)
    mark("do2")
    grad_heads((left, right, other[0], other[1]))

    def grad_weight(r, c):
        chip = lax.rem(x + r, CHIPS)
        part = mm(hot[...], ag[chip * 2 + c].reshape(NB * SPAN, 256)).astype(BF)
        for i in range(2):
            wa[2 * c + i, chip] = part[:HDIM, cols_of(i)]
            wb[chip, 2 * c + i] = part[HDIM:, cols_of(i)]

    mark("gwpart")
    for b in range(NB):
        hot[:, rows_of(b)] = ho[rows_of(b), :].T
    for r in (0, 1, 3):
        grad_weight(r, 0)
        grad_weight(r, 1)
    mark("take3")
    for kind, b in ((2, 1), (2, 3)):
        take(kind, b)
    mark("rs2")
    from_twin(2)
    for b in range(NB):
        x2o[b] = chip_sum(2, b).astype(BF)
    for b in (0, 2, 1, 3):
        push(x2o.at[b], x2i.at[b], send_s.at[10], far_r.at[0], (me, right if b < 2 else left))
    from_twin(1)
    from_twin(3)
    for b in (2, 3):
        xpo[b] = chip_sum(1, b).astype(BF)
        xmo[3 - b] = chip_sum(3, 3 - b).astype(BF)
    for b in (2, 3):
        push(xpo.at[b], xli.at[b], send_s.at[11], far_r.at[1], (me, right))
        push(xmo.at[3 - b], xri.at[3 - b], send_s.at[12], far_r.at[2], (me, left))
    mark("agtwin")
    twin_took(3)
    mark("do3")
    grad_heads((far, other[2]))
    do[...] = dacc[...].astype(BF)
    mark("gwfar")
    grad_weight(2, 0)
    grad_weight(2, 1)

    def along_z(d):
        return y * 4 + lax.rem(z + d, 4)

    def along_y(d):
        return lax.rem(y + d, 4) * 4 + z

    def round_send(src_a, dst_a, src_b, dst_b, i, swap):
        to_a, to_b = (along_y, along_z) if swap else (along_z, along_y)
        at_a, at_b = (y, z) if swap else (z, y)
        for d in range(1, 4):
            push(src_a.at[lax.rem(at_a + d, 4)], dst_a.at[at_a], send_s.at[13 + i], gw_r.at[i], (to_a(d), hd))
            push(src_b.at[lax.rem(at_b + d, 4)], dst_b.at[at_b], send_s.at[14 + i], gw_r.at[i + 1], (to_b(d), hd))

    def round_wait(dst_a, dst_b, i):
        arrived(dst_a.at[pl.ds(0, 3)], gw_r.at[i])
        arrived(dst_b.at[pl.ds(0, 3)], gw_r.at[i + 1])

    def four(ref):
        return (ref[0].astype(F32) + ref[1].astype(F32)) + (ref[2].astype(F32) + ref[3].astype(F32))

    round_send(wa, ga, wb, gb, 0, False)
    ga[z] = wa[z]
    gb[y] = wb[y]

    mark("bwd1")
    for p in range(NP):
        b, h = divmod(p, NH)
        qb = q_ref[rows_of(b), cols_of(h)]
        kb = k_ref[rows_of(b), cols_of(h)]
        vb = v_ref[rows_of(b), cols_of(h)]
        dob = do[rows_of(b), cols_of(h)]
        dsh = causal(mm_nt(dob, vb)).astype(BF)
        ds[p] = dsh
        dsolved = mm(lanes(dsh, dob, dob), rows(kb, mem_h[p], mem_l[p])).astype(BF)
        dv[p] = dsolved
        dinv = mm_tn(qb, dsolved)
        dinv = -scale_s[p][:1, :1] * (dinv + dinv.T)
        dt[0, p] = lanes(dinv.astype(BF), jnp.zeros((HDIM, HDIM), BF))
        tan_s[p] = jnp.zeros((HDIM, HDIM), F32)
        both = mm_tn(dob, lanes(sol_h[p], sol_l[p]))
        dm_s[h, b] = both[:, :HDIM] + both[:, HDIM:]

    for h in range(NH):
        pair_sum = (dm_s[h, 0] + dm_s[h, 1]) + (dm_s[h, 2] + dm_s[h, 3])
        pt2[8 * h : 8 * h + 8] = pair_sum.reshape(8, 16, HDIM).astype(BF)
    exchange(pt2, pinbox2, 6)
    pinbox2[me] = pt2[me]

    mark("dual")
    for j in range(NEWTON):
        for p in range(NP):
            high = exh[j, p]
            here = dt[j % 2, p]
            new = mm(lanes(high[:, :HDIM], here[:, :HDIM]), rows(here, high))
            tangent = tan_s[p] + new[:, HDIM:]
            tan_s[p] = tangent
            if j < NEWTON - 1:
                dt[(j + 1) % 2, p] = lanes(new[:, :HDIM].astype(BF), tangent.astype(BF))
            else:
                b, h = divmod(p, NH)
                trace = total(new[:, :HDIM] * unit)
                residual = high_low(exh, exl, p)
                dg_s[h, b] = tangent + (trace * scale_s[p][:1, :1]) * (unit - residual)

    for h in range(NH):
        gram_sum = (dg_s[h, 0] + dg_s[h, 1]) + (dg_s[h, 2] + dg_s[h, 3])
        st2[8 * h : 8 * h + 8] = gram_sum.reshape(8, 16, HDIM).astype(BF)
    exchange(st2, inbox2, 2)
    inbox2[me] = st2[me]

    mark("bwd2")
    for p in range(NP):
        b, h = divmod(p, NH)
        dob = do[rows_of(b), cols_of(h)]
        xs = rows(exh[NEWTON, p][:, HDIM:], exl[NEWTON, p][:, HDIM:])
        gq_ref[rows_of(b), cols_of(h)] = mm(lanes(dv[p], dv[p]), xs).astype(BF)
        both = mm_tn(ds[p], lanes(sol_h[p], sol_l[p]))
        own[2, rows_of(b), cols_of(h)] = both[:, :HDIM] + both[:, HDIM:]
        dacc[rows_of(b), cols_of(h)] = mm_tn(sc[p], dob)

    mark("rs3")
    arrived(x2i, far_r.at[0])
    for b in (0, 1):
        xpo[b] = (chip_sum(1, b) + x2i[b].astype(F32)).astype(BF)
        xmo[3 - b] = (chip_sum(3, 3 - b) + x2i[3 - b].astype(F32)).astype(BF)
    for b in (0, 1):
        push(xpo.at[b], xli.at[b], send_s.at[11], far_r.at[1], (me, right))
        push(xmo.at[3 - b], xri.at[3 - b], send_s.at[12], far_r.at[2], (me, left))

    mark("rs4")
    to_twin(0)
    own[0] = partial(0, core)
    send_twin(0)

    mark("pscan")
    exchanged(pinbox2, 6)
    scan(pinbox2, poutb2, reversed(range(CTX)))
    exchange(poutb2, poff2, 7)
    poff2[me] = poutb2[me]

    mark("gw2")
    round_wait(ga, gb, 0)
    for i in range(4):
        sa[i] = ((ga[0, i].astype(F32) + ga[1, i].astype(F32)) + (ga[2, i].astype(F32) + ga[3, i].astype(F32))).astype(BF)
        sb[i] = ((gb[0, i].astype(F32) + gb[1, i].astype(F32)) + (gb[2, i].astype(F32) + gb[3, i].astype(F32))).astype(BF)
    round_send(sa, ra, sb, rb, 2, True)
    ra[y] = sa[y]
    rb[z] = sb[z]

    mark("scan3w")
    exchanged(inbox2, 2)
    mark("scan4s")
    scan(inbox2, outb2, reversed(range(CTX)))
    exchange(outb2, off2, 3)
    off2[me] = outb2[me]

    mark("gw3")
    from_twin(0)
    round_wait(ra, rb, 2)
    gw_ref[:HDIM, :] = four(ra)
    gw_ref[HDIM:, :] = four(rb)

    mark("scan4w")
    exchanged(poff2, 7)
    exchanged(off2, 3)
    mark("final")
    for h in range(NH):
        gram = off2[8 * h : 8 * h + 8].reshape(HDIM, HDIM).astype(F32)
        pair = poff2[8 * h : 8 * h + 8].reshape(HDIM, HDIM).astype(F32)
        for b in reversed(range(NB)):
            here = rows_of(b)
            kb = k_ref[here, cols_of(h)]
            vb = v_ref[here, cols_of(h)]
            rh = pair.astype(BF)
            dk = own[2, here, cols_of(h)] + mm(lanes(kb, vb), rows(gram.astype(BF), rh))
            gk_ref[here, cols_of(h)] = dk.astype(BF)
            gv_ref[here, cols_of(h)] = (dacc[here, cols_of(h)] + mm_nt(kb, rh)).astype(BF)
            gram = gram + dg_s[h, b]
            pair = pair + dm_s[h, b]

    mark("lofin")
    arrived(xli, far_r.at[1])
    arrived(xri, far_r.at[2])
    for b in range(NB):
        value = chip_sum(0, b) + xli[b].astype(F32) + xri[b].astype(F32)
        lo_ref[rows_of(b), :] = value.astype(BF)

    mark("waitsend")
    most = pl.ds(0, CTX - 1)
    for i, src in enumerate((st, outb, st2, outb2, pt, poutb, pt2, poutb2)):
        left_here(src.at[most], send_s.at[i])
    left_here(ag.at[pl.ds(0, 7)], send_s.at[8])
    for i, src in enumerate((d2o, x2o, xpo, xmo)):
        left_here(src, send_s.at[9 + i])
    for i, src in enumerate((wa, wb, sa, sb)):
        left_here(src.at[pl.ds(0, 3)], send_s.at[13 + i])
    mark()


def write_out(*refs):
    sources, targets, sems = refs[:5], refs[5:10], refs[10]
    copies = [
        pltpu.make_async_copy(src, dst, sems.at[i])
        for i, (src, dst) in enumerate(zip(sources, targets))
    ]
    for copy in copies:
        copy.start()
    for copy in copies:
        copy.wait()


def shards(queries, keys, values, w_out, cotangent):
    tok = jax.ShapeDtypeStruct((NB * SPAN, NH * HDIM), BF)
    shapes = (tok, tok, tok, tok, jax.ShapeDtypeStruct((256, HDIM), F32))
    vm = lambda *shape: pltpu.VMEM(shape, BF)
    vf = lambda *shape: pltpu.VMEM(shape, F32)
    dma = lambda *shape: pltpu.SemaphoreType.DMA(shape)
    span = pl.BlockSpec(memory_space=pltpu.VMEM)
    anywhere = pl.BlockSpec(memory_space=pl.ANY)
    chunk = [vm(NB, SPAN, 256)]
    flat = [vm(NB * SPAN, 256)]
    scratch = (
        flat * 3 + [vm(256, 2048)] + flat
        + [vm(8, NB, SPAN, 256)]
        + ([vf(CTX, 16, HDIM)] * 4 + [vm(CTX, 16, HDIM)] * 4) * 2
        + [vf(NH, NB, HDIM, HDIM)] * 2
        + [vm(NEWTON + 1, NP, HDIM, 256)] * 2
        + [vm(2, NP, HDIM, 256), vf(NP, HDIM, HDIM)]
        + [vf(NP, 8, HDIM)]
        + [vm(NP, HDIM, HDIM)] * 4
        + [vm(NP, SPAN, HDIM)] * 2
        + [vm(NP, SPAN, SPAN)] * 2
        + [vm(NP, SPAN, HDIM)]
        + flat + [vm(256, NB * SPAN), vf(NB * SPAN, 256)] + flat
        + [vf(NH, NB, HDIM, HDIM)] * 2
        + [vm(CHIPS, NB * SPAN, 256)] * 2
        + [vf(CHIPS, NB * SPAN, 256)]
        + chunk * 6
        + [vm(4, 4, HDIM, HDIM)] * 4
        + [vm(4, HDIM, HDIM)] * 4
        + [dma(5)]
        + [dma(17), dma(8), dma(3, NB), dma(4), dma(4), dma(CHIPS), dma(3)]
    )
    results = pl.pallas_call(
        kernel,
        out_shape=shapes,
        in_specs=[pl.BlockSpec(memory_space=pltpu.HBM)] * 5,
        out_specs=[span] * 5,
        scratch_shapes=scratch,
        compiler_params=pltpu.CompilerParams(
            collective_id=0, has_side_effects=True, vmem_limit_bytes=VMEM_LIMIT
        ),
        name="mesa_layer",
    )(queries, keys, values, w_out, cotangent)
    return pl.pallas_call(
        write_out,
        out_shape=shapes,
        in_specs=[span] * 5,
        out_specs=[anywhere] * 5,
        scratch_shapes=[dma(5)],
        compiler_params=pltpu.CompilerParams(vmem_limit_bytes=1 * 1024 * 1024),
        name="write_out",
    )(*results)


def solution(mesh):
    placed = (P("ctx", "head"), P("ctx", "head"), P("ctx", "head"), P("head", None), P("ctx", "head"))
    return jax.shard_map(
        shards,
        mesh=mesh,
        in_specs=placed,
        out_specs=(P("ctx", "head"), P("ctx", "head"), P("ctx", "head"), P("ctx", "head"), P("head", "ctx")),
        check_vma=False,
    )
```

```python
import jax
import jax.numpy as jnp
from jax import lax
from jax.experimental import pallas as pl
from jax.experimental.pallas import tpu as pltpu
from jax.sharding import PartitionSpec as P

HDIM = 128
SPAN = 256
NEWTON = 8
RIDGE = 1.0
NB = 4
NH = 2
NP = NB * NH
CTX = 16
CHIPS = 4
VMEM_LIMIT = 103 * 512 * 1024
F32 = jnp.float32
BF = jnp.bfloat16
MESH = pl.DeviceIdType.MESH


def mm(a, b):
    return lax.dot_general(a, b, (((1,), (0,)), ((), ())), preferred_element_type=F32)


def mm_nt(a, b):
    return lax.dot_general(a, b, (((1,), (1,)), ((), ())), preferred_element_type=F32)


def mm_tn(a, b):
    return lax.dot_general(a, b, (((0,), (0,)), ((), ())), preferred_element_type=F32)


def rows(*parts):
    return jnp.concatenate(parts, axis=0)


def lanes(*parts):
    return jnp.concatenate(parts, axis=1)


def halves(value):
    high = value.astype(BF)
    return high, (value - high.astype(F32)).astype(BF)


def total(value):
    return jnp.sum(jnp.sum(value, axis=1, keepdims=True), axis=0, keepdims=True)


def eye():
    shape = (HDIM, HDIM)
    return (
        lax.broadcasted_iota(jnp.int32, shape, 0) == lax.broadcasted_iota(jnp.int32, shape, 1)
    ).astype(F32)


def high_low(high, low, p):
    return high[0, p][:, :HDIM].astype(F32) + low[0, p][:, :HDIM].astype(F32)


def causal(value):
    shape = (SPAN, SPAN)
    keep = lax.broadcasted_iota(jnp.int32, shape, 0) >= lax.broadcasted_iota(jnp.int32, shape, 1)
    return jnp.where(keep, value, 0.0)


def kernel(
    q_hbm, k_hbm, v_hbm, w_hbm, cot_hbm,
    lo_ref, gq_ref, gk_ref, gv_ref, gw_ref,
    q_ref, k_ref, v_ref, w_ref, cot_ref,
    ag, st, inbox, outb, off, st2, inbox2, outb2, off2,
    pt, pinbox, poutb, poff, pt2, pinbox2, poutb2, poff2,
    gram_s, pair_s, exh, exl, dt, tan_s, scale_s, mem_h, mem_l, memt_h, memt_l,
    sol_h, sol_l, sc, ds, dv, ho, hot, dacc, do, dg_s, dm_s,
    d2o, d2i, own, x2o, x2i, xpo, xmo, xli, xri, wa, wb, ga, gb, sa, sb, ra, rb,
    in_s, send_s, ex_r, near_r, twin_r, gw_r, d2_r, far_r,
):
    me = lax.axis_index("ctx")
    hd = lax.axis_index("head")
    x = lax.div(hd, 2)
    y = lax.div(me, 4)
    z = lax.rem(me, 4)
    core = lax.rem(hd, 2)
    right = lax.rem(x + 1, CHIPS) * 2 + core
    left = lax.rem(x + 3, CHIPS) * 2 + core
    far = lax.rem(x + 2, CHIPS) * 2 + core
    twin = x * 2 + 1 - core
    other = (left + 1 - 2 * core, right + 1 - 2 * core, far + 1 - 2 * core)
    scope = []

    def mark(name=None):
        if scope:
            scope.pop().__exit__(None, None, None)
        if name is not None:
            now = jax.named_scope(name)
            now.__enter__()
            scope.append(now)

    def remote(src, dst, ss, rs, dev):
        return pltpu.make_async_remote_copy(
            src_ref=src, dst_ref=dst, send_sem=ss, recv_sem=rs, device_id=dev, device_id_type=MESH
        )

    def push(src, dst, ss, rs, dev):
        remote(src, dst, ss, rs, dev).start()

    def arrived(dst, rs):
        remote(dst, dst, send_s.at[0], rs, (me, twin)).wait_recv()

    def left_here(src, ss):
        remote(src, src, ss, ex_r.at[0], (me, twin)).wait_send()

    def exchange(src, dst, i):
        for d in range(1, CTX):
            peer = lax.rem(me + d, CTX)
            push(src.at[peer], dst.at[me], send_s.at[i], ex_r.at[i], (peer, hd))

    def exchanged(dst, i):
        arrived(dst.at[pl.ds(0, CTX - 1)], ex_r.at[i])

    def rows_of(b):
        return slice(b * SPAN, (b + 1) * SPAN)

    def cols_of(h):
        return slice(h * HDIM, (h + 1) * HDIM)

    mark("entry")
    barrier = pltpu.get_barrier_semaphore()
    for d in range(1, CTX):
        pl.semaphore_signal(barrier, inc=1, device_id=(lax.rem(me + d, CTX), hd), device_id_type=MESH)
    for dev in (right, left, twin):
        pl.semaphore_signal(barrier, inc=1, device_id=(me, dev), device_id_type=MESH)
    loads = [
        pltpu.make_async_copy(src, dst, in_s.at[i])
        for i, (src, dst) in enumerate(
            ((k_hbm, k_ref), (v_hbm, v_ref), (cot_hbm, cot_ref), (q_hbm, q_ref), (w_hbm, w_ref))
        )
    ]
    for load in loads[:3]:
        load.start()

    loads[0].wait()
    loads[1].wait()
    for load in loads[3:]:
        load.start()
    mark("gram")
    for h in range(NH):
        gram_sum = jnp.zeros((HDIM, HDIM), F32)
        pair_sum = jnp.zeros((HDIM, HDIM), F32)
        for b in range(NB):
            kb = k_ref[rows_of(b), cols_of(h)]
            vb = v_ref[rows_of(b), cols_of(h)]
            gram = mm_tn(kb, kb)
            pair = mm_tn(vb, kb)
            gram_s[h, b] = gram
            pair_s[h, b] = pair
            gram_sum = gram_sum + gram
            pair_sum = pair_sum + pair
        st[8 * h : 8 * h + 8] = gram_sum.reshape(8, 16, HDIM)
        pt[8 * h : 8 * h + 8] = pair_sum.reshape(8, 16, HDIM)
    inbox[me] = st[me]
    pinbox[me] = pt[me]
    loads[2].wait()
    mark("barrier")
    pl.semaphore_wait(barrier, CTX - 1 + 3)

    exchange(st, inbox, 0)
    for b in range(NB):
        for kind, dev, blk in ((0, right, b), (1, left, (b + 2) % NB)):
            push(
                cot_ref.at[pl.ds(blk * SPAN, SPAN), :], ag.at[hd, blk],
                send_s.at[8], near_r.at[kind, blk], (me, dev),
            )
    for b in range(NB):
        push(
            cot_ref.at[pl.ds(b * SPAN, SPAN), :], ag.at[hd, b],
            send_s.at[8], twin_r.at[0], (me, twin),
        )
        ag[hd, b] = cot_ref[rows_of(b), :]
    exchange(pt, pinbox, 4)

    def take(kind, b, relay=None):
        shard = (left, right, far)[kind]
        here = ag.at[shard, b]
        arrived(here, near_r.at[kind, b])
        if relay is not None:
            push(here, here, send_s.at[8], near_r.at[2, b], (me, relay))
        push(here, here, send_s.at[8], twin_r.at[1 + kind], (me, twin))

    def scan(box, out, order):
        run = jnp.zeros((16, HDIM), F32)
        for i in order:
            out[i] = run.astype(out.dtype)
            run = run + box[i].astype(F32)

    def twin_took(kind):
        arrived(ag.at[(twin, *other)[kind]], twin_r.at[kind])

    def grad_heads(ids, start=False):
        for b in range(NB):
            acc = None if start else dacc[rows_of(b), :]
            for s in ids:
                cols = pl.ds(pl.multiple_of(s * 256, 256), 256)
                part = mm_nt(ag[s, b], w_ref[:, cols])
                acc = part if acc is None else acc + part
            dacc[rows_of(b), :] = acc

    unit = eye()
    loads[3].wait()
    loads[4].wait()
    mark("scan1w")
    exchanged(inbox, 0)
    mark("scan2s")
    scan(inbox, outb, range(CTX))
    exchange(outb, off, 1)
    off[me] = outb[me]
    exchanged(pinbox, 4)
    scan(pinbox, poutb, range(CTX))
    exchange(poutb, poff, 5)
    poff[me] = poutb[me]
    mark("relay")
    take(0, 0, right)
    take(1, 2, left)
    twin_took(0)
    mark("do1")
    grad_heads((hd, twin), True)
    mark("scan2w")
    exchanged(off, 1)

    mark("newton")
    for h in range(NH):
        gram = off[8 * h : 8 * h + 8].reshape(HDIM, HDIM)
        for b in range(NB):
            p = b * NH + h
            ridged = gram + RIDGE * unit
            scale = 1.0 / jnp.sqrt(total(ridged * ridged))
            eh, el = halves(unit - scale * ridged)
            xh, xl = halves(scale * unit)
            exh[0, p] = lanes(eh, xh)
            exl[0, p] = lanes(el, xl)
            scale_s[p] = jnp.broadcast_to(scale, (8, HDIM))
            gram = gram + gram_s[h, b]

    for j in range(NEWTON):
        if j == 3:
            take(0, 1, right)
            take(1, 3, left)
        for p in range(NP):
            high = exh[j, p]
            low = exl[j, p]
            eh = high[:, :HDIM]
            el = low[:, :HDIM]
            new = mm(lanes(eh, el, eh), rows(high, high, low))
            iterate = high[:, HDIM:].astype(F32) + low[:, HDIM:].astype(F32) + new[:, HDIM:]
            nh, nl = halves(lanes(new[:, :HDIM], iterate))
            exh[j + 1, p] = nh
            exl[j + 1, p] = nl

    mark("take1")
    take(0, 2)
    take(1, 0)
    mark("pair")
    exchanged(poff, 5)
    for h in range(NH):
        pair = poff[8 * h : 8 * h + 8].reshape(HDIM, HDIM)
        for b in range(NB):
            p = b * NH + h
            mem_h[p], mem_l[p] = halves(pair)
            memt_h[p], memt_l[p] = halves(pair.T)
            pair = pair + pair_s[h, b]

    mark("forward")
    for p in range(NP):
        if p == 5:
            take(0, 3)
            take(1, 1)
        b, h = divmod(p, NH)
        qb = q_ref[rows_of(b), cols_of(h)]
        kb = k_ref[rows_of(b), cols_of(h)]
        vb = v_ref[rows_of(b), cols_of(h)]
        xh = exh[NEWTON, p][:, HDIM:]
        xl = exl[NEWTON, p][:, HDIM:]
        sh, sl = halves(mm(lanes(qb, qb), rows(xh, xl)))
        sol_h[p] = sh
        sol_l[p] = sl
        ch = causal(mm_nt(lanes(sh, sl), lanes(kb, kb))).astype(BF)
        sc[p] = ch
        out = mm(lanes(ch, sh, sh), rows(vb, memt_h[p], memt_l[p]))
        ho[rows_of(b), cols_of(h)] = out.astype(BF)

    def partial(r, c):
        dest = lax.rem(x + r, CHIPS) * 2 + c
        return mm(ho[...], w_ref[:, pl.ds(pl.multiple_of(dest * 256, 256), 256)])

    def to_twin(r):
        d2o[r] = partial(r, 1 - core).astype(BF)

    def send_twin(r):
        push(d2o.at[r], d2i.at[r], send_s.at[9], d2_r.at[r], (me, twin))

    def from_twin(r):
        arrived(d2i.at[r], d2_r.at[r])

    def chip_sum(r, b):
        return own[r, rows_of(b), :] + d2i[r, rows_of(b), :].astype(F32)

    mark("rs1")
    to_twin(2)
    for b in (0, 2, 1, 3):
        part = d2o.at[2, pl.ds(b * SPAN, SPAN), :]
        push(part, d2i.at[2, pl.ds(b * SPAN, SPAN), :], send_s.at[9], d2_r.at[2 if b in (0, 2) else 4], (me, twin))
    own[2] = partial(2, core)
    to_twin(1)
    to_twin(3)
    send_twin(1)
    send_twin(3)
    mark("rs2b")
    own[1] = partial(1, core)
    own[3] = partial(3, core)
    mark("rs2")
    for i, pair in ((2, (0, 2)), (4, (1, 3))):
        arrived(d2i.at[2, pl.ds(0, 2 * SPAN), :], d2_r.at[i])
        for b in pair:
            x2o[b] = chip_sum(2, b).astype(BF)
        for b in pair:
            push(x2o.at[b], x2i.at[b], send_s.at[10], far_r.at[0], (me, right if b < 2 else left))
    mark("take2b")
    for kind, b in ((2, 0), (2, 2)):
        take(kind, b)
    mark("take3")
    for kind, b in ((2, 1), (2, 3)):
        take(kind, b)
    mark("take4")
    twin_took(1)
    twin_took(2)
    mark("do2")
    grad_heads((left, right, other[0], other[1]))

    def along_z(d):
        return y * 4 + lax.rem(z + d, 4)

    def along_y(d):
        return lax.rem(y + d, 4) * 4 + z

    def grad_weight(r, c):
        chip = lax.rem(x + r, CHIPS)
        part = mm(hot[...], ag[chip * 2 + c].reshape(NB * SPAN, 256)).astype(BF)
        for i in range(2):
            wa[2 * c + i, chip] = part[:HDIM, cols_of(i)]
            wb[chip, 2 * c + i] = part[HDIM:, cols_of(i)]

    mark("gwpart")
    for b in range(NB):
        hot[:, rows_of(b)] = ho[rows_of(b), :].T
    for r in (0, 1, 3):
        grad_weight(r, 0)
        grad_weight(r, 1)
    far_chip = lax.rem(x + 2, CHIPS)

    def first_round(near):
        for d in range(1, 4):
            dest = lax.rem(y + d, 4)
            for r in (0, 1, 3) if near else (2,):
                chip = lax.rem(x + r, CHIPS)
                push(wa.at[lax.rem(z + d, 4), chip], ga.at[z, chip], send_s.at[13], gw_r.at[0], (along_z(d), hd))

            @pl.when((dest != far_chip) if near else (dest == far_chip))
            def _():
                push(wb.at[dest], gb.at[y], send_s.at[14], gw_r.at[1], (along_y(d), hd))

    first_round(True)
    mark("rs2c")
    from_twin(1)
    from_twin(3)
    for b in (2, 3):
        xpo[b] = chip_sum(1, b).astype(BF)
        xmo[3 - b] = chip_sum(3, 3 - b).astype(BF)
    for b in (2, 3):
        push(xpo.at[b], xli.at[b], send_s.at[11], far_r.at[1], (me, right))
        push(xmo.at[3 - b], xri.at[3 - b], send_s.at[12], far_r.at[2], (me, left))
    mark("agtwin")
    twin_took(3)
    mark("do3")
    grad_heads((far, other[2]))
    do[...] = dacc[...].astype(BF)
    mark("gwfar")
    grad_weight(2, 0)
    grad_weight(2, 1)

    def second_round():
        for d in range(1, 4):
            push(sa.at[lax.rem(y + d, 4)], ra.at[y], send_s.at[15], gw_r.at[2], (along_y(d), hd))
            push(sb.at[lax.rem(z + d, 4)], rb.at[z], send_s.at[16], gw_r.at[3], (along_z(d), hd))

    def round_wait(dst_a, dst_b, i):
        arrived(dst_a.at[pl.ds(0, 3)], gw_r.at[i])
        arrived(dst_b.at[pl.ds(0, 3)], gw_r.at[i + 1])

    def four(ref):
        return (ref[0].astype(F32) + ref[1].astype(F32)) + (ref[2].astype(F32) + ref[3].astype(F32))

    first_round(False)
    ga[z] = wa[z]
    gb[y] = wb[y]

    mark("bwd1")
    for p in range(NP):
        b, h = divmod(p, NH)
        qb = q_ref[rows_of(b), cols_of(h)]
        kb = k_ref[rows_of(b), cols_of(h)]
        vb = v_ref[rows_of(b), cols_of(h)]
        dob = do[rows_of(b), cols_of(h)]
        dsh = causal(mm_nt(dob, vb)).astype(BF)
        ds[p] = dsh
        dsolved = mm(lanes(dsh, dob, dob), rows(kb, mem_h[p], mem_l[p])).astype(BF)
        dv[p] = dsolved
        dinv = mm_tn(qb, dsolved)
        dinv = -scale_s[p][:1, :1] * (dinv + dinv.T)
        dt[0, p] = lanes(dinv.astype(BF), jnp.zeros((HDIM, HDIM), BF))
        tan_s[p] = jnp.zeros((HDIM, HDIM), F32)
        both = mm_tn(dob, lanes(sol_h[p], sol_l[p]))
        dm_s[h, b] = both[:, :HDIM] + both[:, HDIM:]

    for h in range(NH):
        pair_sum = (dm_s[h, 0] + dm_s[h, 1]) + (dm_s[h, 2] + dm_s[h, 3])
        pt2[8 * h : 8 * h + 8] = pair_sum.reshape(8, 16, HDIM).astype(BF)
    exchange(pt2, pinbox2, 6)
    pinbox2[me] = pt2[me]

    mark("dual")
    for j in range(NEWTON):
        for p in range(NP):
            high = exh[j, p]
            here = dt[j % 2, p]
            new = mm(lanes(high[:, :HDIM], here[:, :HDIM]), rows(here, high))
            tangent = tan_s[p] + new[:, HDIM:]
            tan_s[p] = tangent
            if j < NEWTON - 1:
                dt[(j + 1) % 2, p] = lanes(new[:, :HDIM].astype(BF), tangent.astype(BF))
            else:
                b, h = divmod(p, NH)
                trace = total(new[:, :HDIM] * unit)
                residual = high_low(exh, exl, p)
                dg_s[h, b] = tangent + (trace * scale_s[p][:1, :1]) * (unit - residual)

    for h in range(NH):
        gram_sum = (dg_s[h, 0] + dg_s[h, 1]) + (dg_s[h, 2] + dg_s[h, 3])
        st2[8 * h : 8 * h + 8] = gram_sum.reshape(8, 16, HDIM).astype(BF)
    exchange(st2, inbox2, 2)
    inbox2[me] = st2[me]

    mark("rs3")
    arrived(x2i, far_r.at[0])
    for b in (0, 1):
        xpo[b] = (chip_sum(1, b) + x2i[b].astype(F32)).astype(BF)
        xmo[3 - b] = (chip_sum(3, 3 - b) + x2i[3 - b].astype(F32)).astype(BF)
    for b in (0, 1):
        push(xpo.at[b], xli.at[b], send_s.at[11], far_r.at[1], (me, right))
        push(xmo.at[3 - b], xri.at[3 - b], send_s.at[12], far_r.at[2], (me, left))

    mark("bwd2")
    for p in range(NP):
        b, h = divmod(p, NH)
        dob = do[rows_of(b), cols_of(h)]
        xs = rows(exh[NEWTON, p][:, HDIM:], exl[NEWTON, p][:, HDIM:])
        gq_ref[rows_of(b), cols_of(h)] = mm(lanes(dv[p], dv[p]), xs).astype(BF)
        both = mm_tn(ds[p], lanes(sol_h[p], sol_l[p]))
        own[2, rows_of(b), cols_of(h)] = both[:, :HDIM] + both[:, HDIM:]
        dacc[rows_of(b), cols_of(h)] = mm_tn(sc[p], dob)

    mark("rs4")
    to_twin(0)
    own[0] = partial(0, core)
    send_twin(0)

    mark("pscan")
    exchanged(pinbox2, 6)
    scan(pinbox2, poutb2, reversed(range(CTX)))
    exchange(poutb2, poff2, 7)
    poff2[me] = poutb2[me]

    mark("scan3w")
    exchanged(inbox2, 2)
    mark("scan4s")
    scan(inbox2, outb2, reversed(range(CTX)))
    exchange(outb2, off2, 3)
    off2[me] = outb2[me]

    mark("gw2")
    round_wait(ga, gb, 0)
    for i in range(4):
        sa[i] = ((ga[0, i].astype(F32) + ga[1, i].astype(F32)) + (ga[2, i].astype(F32) + ga[3, i].astype(F32))).astype(BF)
        sb[i] = ((gb[0, i].astype(F32) + gb[1, i].astype(F32)) + (gb[2, i].astype(F32) + gb[3, i].astype(F32))).astype(BF)
    second_round()
    ra[y] = sa[y]
    rb[z] = sb[z]

    mark("gw3")
    from_twin(0)
    round_wait(ra, rb, 2)
    gw_ref[:HDIM, :] = four(ra)
    gw_ref[HDIM:, :] = four(rb)

    mark("scan4w")
    exchanged(poff2, 7)
    exchanged(off2, 3)
    mark("final")
    for h in range(NH):
        gram = off2[8 * h : 8 * h + 8].reshape(HDIM, HDIM).astype(F32)
        pair = poff2[8 * h : 8 * h + 8].reshape(HDIM, HDIM).astype(F32)
        for b in reversed(range(NB)):
            here = rows_of(b)
            kb = k_ref[here, cols_of(h)]
            vb = v_ref[here, cols_of(h)]
            rh = pair.astype(BF)
            dk = own[2, here, cols_of(h)] + mm(lanes(kb, vb), rows(gram.astype(BF), rh))
            gk_ref[here, cols_of(h)] = dk.astype(BF)
            gv_ref[here, cols_of(h)] = (dacc[here, cols_of(h)] + mm_nt(kb, rh)).astype(BF)
            gram = gram + dg_s[h, b]
            pair = pair + dm_s[h, b]

    mark("lofin")
    arrived(xli, far_r.at[1])
    arrived(xri, far_r.at[2])
    for b in range(NB):
        value = chip_sum(0, b) + xli[b].astype(F32) + xri[b].astype(F32)
        lo_ref[rows_of(b), :] = value.astype(BF)

    mark("waitsend")
    most = pl.ds(0, CTX - 1)
    for i, src in enumerate((st, outb, st2, outb2, pt, poutb, pt2, poutb2)):
        left_here(src.at[most], send_s.at[i])
    left_here(ag.at[pl.ds(0, 7)], send_s.at[8])
    for i, src in enumerate((d2o, x2o, xpo, xmo)):
        left_here(src, send_s.at[9 + i])
    for i, src in enumerate((wa, wb, sa, sb)):
        left_here(src.at[pl.ds(0, 3)], send_s.at[13 + i])
    mark()


def write_out(*refs):
    sources, targets, sems = refs[:5], refs[5:10], refs[10]
    copies = [
        pltpu.make_async_copy(src, dst, sems.at[i])
        for i, (src, dst) in enumerate(zip(sources, targets))
    ]
    for copy in copies:
        copy.start()
    for copy in copies:
        copy.wait()


def shards(queries, keys, values, w_out, cotangent):
    tok = jax.ShapeDtypeStruct((NB * SPAN, NH * HDIM), BF)
    shapes = (tok, tok, tok, tok, jax.ShapeDtypeStruct((256, HDIM), F32))
    vm = lambda *shape: pltpu.VMEM(shape, BF)
    vf = lambda *shape: pltpu.VMEM(shape, F32)
    dma = lambda *shape: pltpu.SemaphoreType.DMA(shape)
    span = pl.BlockSpec(memory_space=pltpu.VMEM)
    anywhere = pl.BlockSpec(memory_space=pl.ANY)
    chunk = [vm(NB, SPAN, 256)]
    flat = [vm(NB * SPAN, 256)]
    scratch = (
        flat * 3 + [vm(256, 2048)] + flat
        + [vm(8, NB, SPAN, 256)]
        + ([vf(CTX, 16, HDIM)] * 4 + [vm(CTX, 16, HDIM)] * 4) * 2
        + [vf(NH, NB, HDIM, HDIM)] * 2
        + [vm(NEWTON + 1, NP, HDIM, 256)] * 2
        + [vm(2, NP, HDIM, 256), vf(NP, HDIM, HDIM)]
        + [vf(NP, 8, HDIM)]
        + [vm(NP, HDIM, HDIM)] * 4
        + [vm(NP, SPAN, HDIM)] * 2
        + [vm(NP, SPAN, SPAN)] * 2
        + [vm(NP, SPAN, HDIM)]
        + flat + [vm(256, NB * SPAN), vf(NB * SPAN, 256)] + flat
        + [vf(NH, NB, HDIM, HDIM)] * 2
        + [vm(CHIPS, NB * SPAN, 256)] * 2
        + [vf(CHIPS, NB * SPAN, 256)]
        + chunk * 6
        + [vm(4, 4, HDIM, HDIM)] * 4
        + [vm(4, HDIM, HDIM)] * 4
        + [dma(5)]
        + [dma(17), dma(8), dma(3, NB), dma(4), dma(4), dma(5), dma(3)]
    )
    results = pl.pallas_call(
        kernel,
        out_shape=shapes,
        in_specs=[pl.BlockSpec(memory_space=pltpu.HBM)] * 5,
        out_specs=[span] * 5,
        scratch_shapes=scratch,
        compiler_params=pltpu.CompilerParams(
            collective_id=0, has_side_effects=True, vmem_limit_bytes=VMEM_LIMIT
        ),
        name="mesa_layer",
    )(queries, keys, values, w_out, cotangent)
    return pl.pallas_call(
        write_out,
        out_shape=shapes,
        in_specs=[span] * 5,
        out_specs=[anywhere] * 5,
        scratch_shapes=[dma(5)],
        compiler_params=pltpu.CompilerParams(vmem_limit_bytes=1 * 1024 * 1024),
        name="write_out",
    )(*results)


def solution(mesh):
    placed = (P("ctx", "head"), P("ctx", "head"), P("ctx", "head"), P("head", None), P("ctx", "head"))
    return jax.shard_map(
        shards,
        mesh=mesh,
        in_specs=placed,
        out_specs=(P("ctx", "head"), P("ctx", "head"), P("ctx", "head"), P("ctx", "head"), P("head", "ctx")),
        check_vma=False,
    )
```

```python
import jax
import jax.numpy as jnp
from jax import lax
from jax.experimental import pallas as pl
from jax.experimental.pallas import tpu as pltpu
from jax.sharding import PartitionSpec as P

HDIM = 128
SPAN = 256
NEWTON = 8
RIDGE = 1.0
NB = 4
NH = 2
NP = NB * NH
CTX = 16
CHIPS = 4
VMEM_LIMIT = 103 * 512 * 1024
F32 = jnp.float32
BF = jnp.bfloat16
MESH = pl.DeviceIdType.MESH


def mm(a, b):
    return lax.dot_general(a, b, (((1,), (0,)), ((), ())), preferred_element_type=F32)


def mm_nt(a, b):
    return lax.dot_general(a, b, (((1,), (1,)), ((), ())), preferred_element_type=F32)


def mm_tn(a, b):
    return lax.dot_general(a, b, (((0,), (0,)), ((), ())), preferred_element_type=F32)


def rows(*parts):
    return jnp.concatenate(parts, axis=0)


def lanes(*parts):
    return jnp.concatenate(parts, axis=1)


def halves(value):
    high = value.astype(BF)
    return high, (value - high.astype(F32)).astype(BF)


def total(value):
    return jnp.sum(jnp.sum(value, axis=1, keepdims=True), axis=0, keepdims=True)


def eye():
    shape = (HDIM, HDIM)
    return (
        lax.broadcasted_iota(jnp.int32, shape, 0) == lax.broadcasted_iota(jnp.int32, shape, 1)
    ).astype(F32)


def high_low(high, low, p):
    return high[0, p][:, :HDIM].astype(F32) + low[0, p][:, :HDIM].astype(F32)


def causal(value):
    shape = (SPAN, SPAN)
    keep = lax.broadcasted_iota(jnp.int32, shape, 0) >= lax.broadcasted_iota(jnp.int32, shape, 1)
    return jnp.where(keep, value, 0.0)


def kernel(
    q_hbm, k_hbm, v_hbm, w_hbm, cot_hbm,
    lo_ref, gq_ref, gk_ref, gv_ref, gw_ref,
    q_ref, k_ref, v_ref, w_ref, cot_ref,
    ag, st, inbox, outb, off, st2, inbox2, outb2, off2,
    pt, pinbox, poutb, poff, pt2, pinbox2, poutb2, poff2,
    gram_s, pair_s, exh, exl, dt, tan_s, scale_s, inv_h, inv_l, mem_h, mem_l, memt_h, memt_l,
    sol_h, sol_l, sc, ds, dv_h, dv_l, ho, hot, dacc, do, dg_s, dm_s,
    d2o, d2i, own, x2o, x2i, xpo, xmo, xli, xri, wa, wb, ga, gb, sa, sb, ra, rb,
    in_s, send_s, ex_r, near_r, twin_r, gw_r, d2_r, far_r,
):
    me = lax.axis_index("ctx")
    hd = lax.axis_index("head")
    x = lax.div(hd, 2)
    y = lax.div(me, 4)
    z = lax.rem(me, 4)
    core = lax.rem(hd, 2)
    right = lax.rem(x + 1, CHIPS) * 2 + core
    left = lax.rem(x + 3, CHIPS) * 2 + core
    far = lax.rem(x + 2, CHIPS) * 2 + core
    twin = x * 2 + 1 - core
    other = (left + 1 - 2 * core, right + 1 - 2 * core, far + 1 - 2 * core)
    scope = []

    def mark(name=None):
        if scope:
            scope.pop().__exit__(None, None, None)
        if name is not None:
            now = jax.named_scope(name)
            now.__enter__()
            scope.append(now)

    def remote(src, dst, ss, rs, dev):
        return pltpu.make_async_remote_copy(
            src_ref=src, dst_ref=dst, send_sem=ss, recv_sem=rs, device_id=dev, device_id_type=MESH
        )

    def push(src, dst, ss, rs, dev):
        remote(src, dst, ss, rs, dev).start()

    def arrived(dst, rs):
        remote(dst, dst, send_s.at[0], rs, (me, twin)).wait_recv()

    def left_here(src, ss):
        remote(src, src, ss, ex_r.at[0], (me, twin)).wait_send()

    def exchange(src, dst, i):
        for d in range(1, CTX):
            peer = lax.rem(me + d, CTX)
            push(src.at[peer], dst.at[me], send_s.at[i], ex_r.at[i], (peer, hd))

    def exchanged(dst, i):
        arrived(dst.at[pl.ds(0, CTX - 1)], ex_r.at[i])

    def rows_of(b):
        return slice(b * SPAN, (b + 1) * SPAN)

    def cols_of(h):
        return slice(h * HDIM, (h + 1) * HDIM)

    mark("entry")
    barrier = pltpu.get_barrier_semaphore()
    for d in range(1, CTX):
        pl.semaphore_signal(barrier, inc=1, device_id=(lax.rem(me + d, CTX), hd), device_id_type=MESH)
    for dev in (right, left, twin):
        pl.semaphore_signal(barrier, inc=1, device_id=(me, dev), device_id_type=MESH)
    loads = [
        pltpu.make_async_copy(src, dst, in_s.at[i])
        for i, (src, dst) in enumerate(
            ((k_hbm, k_ref), (v_hbm, v_ref), (cot_hbm, cot_ref), (q_hbm, q_ref), (w_hbm, w_ref))
        )
    ]
    for load in loads[:3]:
        load.start()

    loads[0].wait()
    loads[1].wait()
    for load in loads[3:]:
        load.start()
    mark("gram")
    for h in range(NH):
        gram_sum = jnp.zeros((HDIM, HDIM), F32)
        pair_sum = jnp.zeros((HDIM, HDIM), F32)
        for b in range(NB):
            kb = k_ref[rows_of(b), cols_of(h)]
            vb = v_ref[rows_of(b), cols_of(h)]
            gram = mm_tn(kb, kb)
            pair = mm_tn(vb, kb)
            gram_s[h, b] = gram
            pair_s[h, b] = pair
            gram_sum = gram_sum + gram
            pair_sum = pair_sum + pair
        st[8 * h : 8 * h + 8] = gram_sum.reshape(8, 16, HDIM)
        pt[8 * h : 8 * h + 8] = pair_sum.reshape(8, 16, HDIM)
    inbox[me] = st[me]
    pinbox[me] = pt[me]
    loads[2].wait()
    mark("barrier")
    pl.semaphore_wait(barrier, CTX - 1 + 3)

    exchange(st, inbox, 0)
    for b in range(NB):
        for kind, dev, blk in ((0, right, b), (1, left, (b + 2) % NB)):
            push(
                cot_ref.at[pl.ds(blk * SPAN, SPAN), :], ag.at[hd, blk],
                send_s.at[8], near_r.at[kind, blk], (me, dev),
            )
    for b in range(NB):
        push(
            cot_ref.at[pl.ds(b * SPAN, SPAN), :], ag.at[hd, b],
            send_s.at[8], twin_r.at[0], (me, twin),
        )
        ag[hd, b] = cot_ref[rows_of(b), :]
    exchange(pt, pinbox, 4)

    def take(kind, b, relay=None):
        shard = (left, right, far)[kind]
        here = ag.at[shard, b]
        arrived(here, near_r.at[kind, b])
        if relay is not None:
            push(here, here, send_s.at[8], near_r.at[2, b], (me, relay))
        push(here, here, send_s.at[8], twin_r.at[1 + kind], (me, twin))

    def scan(box, out, order):
        run = jnp.zeros((16, HDIM), F32)
        for i in order:
            out[i] = run.astype(out.dtype)
            run = run + box[i].astype(F32)

    def twin_took(kind):
        arrived(ag.at[(twin, *other)[kind]], twin_r.at[kind])

    def grad_heads(ids, start=False):
        for b in range(NB):
            acc = None if start else dacc[rows_of(b), :]
            for s in ids:
                cols = pl.ds(pl.multiple_of(s * 256, 256), 256)
                part = mm_nt(ag[s, b], w_ref[:, cols])
                acc = part if acc is None else acc + part
            dacc[rows_of(b), :] = acc

    unit = eye()
    loads[3].wait()
    loads[4].wait()
    mark("scan1w")
    exchanged(inbox, 0)
    mark("scan2s")
    scan(inbox, outb, range(CTX))
    exchange(outb, off, 1)
    off[me] = outb[me]
    exchanged(pinbox, 4)
    scan(pinbox, poutb, range(CTX))
    exchange(poutb, poff, 5)
    poff[me] = poutb[me]
    mark("relay")
    take(0, 0, right)
    take(1, 2, left)
    twin_took(0)
    mark("do1")
    grad_heads((hd, twin), True)
    mark("scan2w")
    exchanged(off, 1)

    mark("newton")
    for h in range(NH):
        gram = off[8 * h : 8 * h + 8].reshape(HDIM, HDIM)
        for b in range(NB):
            p = b * NH + h
            ridged = gram + RIDGE * unit
            scale = 1.0 / jnp.sqrt(total(ridged * ridged))
            eh, el = halves(unit - scale * ridged)
            xh, xl = halves(scale * unit)
            exh[0, p] = lanes(eh, xh)
            exl[0, p] = lanes(el, xl)
            scale_s[p] = jnp.broadcast_to(scale, (8, HDIM))
            gram = gram + gram_s[h, b]

    for j in range(NEWTON):
        if j == 3:
            take(0, 1, right)
            take(1, 3, left)
        for p in range(NP):
            high = exh[j, p]
            low = exl[j, p]
            eh = high[:, :HDIM]
            el = low[:, :HDIM]
            if j == NEWTON - 1:
                xh, xl = high[:, HDIM:], low[:, HDIM:]
                new = mm(lanes(eh, el, eh), rows(xh, xh, xl))
                inv_h[p], inv_l[p] = halves(xh.astype(F32) + xl.astype(F32) + new)
                continue
            new = mm(lanes(eh, el, eh), rows(high, high, low))
            iterate = high[:, HDIM:].astype(F32) + low[:, HDIM:].astype(F32) + new[:, HDIM:]
            nh, nl = halves(lanes(new[:, :HDIM], iterate))
            exh[j + 1, p] = nh
            exl[j + 1, p] = nl

    mark("take1")
    take(0, 2)
    take(1, 0)
    mark("pair")
    exchanged(poff, 5)
    for h in range(NH):
        pair = poff[8 * h : 8 * h + 8].reshape(HDIM, HDIM)
        for b in range(NB):
            p = b * NH + h
            mem_h[p], mem_l[p] = halves(pair)
            memt_h[p], memt_l[p] = halves(pair.T)
            pair = pair + pair_s[h, b]

    mark("forward")
    for p in range(NP):
        if p == 5:
            take(0, 3)
            take(1, 1)
        b, h = divmod(p, NH)
        qb = q_ref[rows_of(b), cols_of(h)]
        kb = k_ref[rows_of(b), cols_of(h)]
        vb = v_ref[rows_of(b), cols_of(h)]
        xh = inv_h[p]
        xl = inv_l[p]
        sh, sl = halves(mm(lanes(qb, qb), rows(xh, xl)))
        sol_h[p] = sh
        sol_l[p] = sl
        ch = causal(mm_nt(lanes(sh, sl), lanes(kb, kb))).astype(BF)
        sc[p] = ch
        out = mm(lanes(ch, sh, sh), rows(vb, memt_h[p], memt_l[p]))
        ho[rows_of(b), cols_of(h)] = out.astype(BF)

    def partial(r, c):
        dest = lax.rem(x + r, CHIPS) * 2 + c
        return mm(ho[...], w_ref[:, pl.ds(pl.multiple_of(dest * 256, 256), 256)])

    def to_twin(r):
        d2o[r] = partial(r, 1 - core).astype(BF)

    def send_twin(r):
        push(d2o.at[r], d2i.at[r], send_s.at[9], d2_r.at[r], (me, twin))

    def from_twin(r):
        arrived(d2i.at[r], d2_r.at[r])

    def chip_sum(r, b):
        return own[r, rows_of(b), :] + d2i[r, rows_of(b), :].astype(F32)

    def send_far():
        for i, pair in ((2, (0, 2)), (4, (1, 3))):
            arrived(d2i.at[2, pl.ds(0, 2 * SPAN), :], d2_r.at[i])
            for b in pair:
                x2o[b] = chip_sum(2, b).astype(BF)
            for b in pair:
                push(x2o.at[b], x2i.at[b], send_s.at[10], far_r.at[0], (me, right if b < 2 else left))

    mark("rs1")
    for b in (0, 2, 1, 3):
        dest = lax.rem(x + 2, CHIPS) * 2 + 1 - core
        wcols = w_ref[:, pl.ds(pl.multiple_of(dest * 256, 256), 256)]
        d2o[2, rows_of(b), :] = mm(ho[rows_of(b), :], wcols).astype(BF)
        if b in (2, 3):
            for i in (b - 2, b):
                part = d2o.at[2, pl.ds(i * SPAN, SPAN), :]
                push(part, d2i.at[2, pl.ds(i * SPAN, SPAN), :], send_s.at[9], d2_r.at[2 if b == 2 else 4], (me, twin))
    own[2] = partial(2, core)
    mark("rs2even")
    pl.when(core == 0)(send_far)
    mark("rs1b")
    to_twin(1)
    to_twin(3)
    send_twin(1)
    send_twin(3)
    mark("rs2b")
    own[1] = partial(1, core)
    own[3] = partial(3, core)
    mark("rs2odd")
    pl.when(core == 1)(send_far)
    mark("take2b")
    for kind, b in ((2, 0), (2, 2)):
        take(kind, b)
    mark("take3")
    for kind, b in ((2, 1), (2, 3)):
        take(kind, b)
    mark("take4")
    twin_took(1)
    twin_took(2)
    mark("do2")
    grad_heads((left, right, other[0], other[1]))

    def along_z(d):
        return y * 4 + lax.rem(z + d, 4)

    def along_y(d):
        return lax.rem(y + d, 4) * 4 + z

    def grad_weight(r, c):
        chip = lax.rem(x + r, CHIPS)
        part = mm(hot[...], ag[chip * 2 + c].reshape(NB * SPAN, 256)).astype(BF)
        for i in range(2):
            wa[2 * c + i, chip] = part[:HDIM, cols_of(i)]
            wb[chip, 2 * c + i] = part[HDIM:, cols_of(i)]

    mark("gwpart")
    for b in range(NB):
        hot[:, rows_of(b)] = ho[rows_of(b), :].T
    for r in (0, 1, 3):
        grad_weight(r, 0)
        grad_weight(r, 1)
    far_chip = lax.rem(x + 2, CHIPS)

    def first_round(near):
        for d in range(1, 4):
            dest = lax.rem(y + d, 4)
            for r in (0, 1, 3) if near else (2,):
                chip = lax.rem(x + r, CHIPS)
                push(wa.at[lax.rem(z + d, 4), chip], ga.at[z, chip], send_s.at[13], gw_r.at[0], (along_z(d), hd))

            @pl.when((dest != far_chip) if near else (dest == far_chip))
            def _():
                push(wb.at[dest], gb.at[y], send_s.at[14], gw_r.at[1], (along_y(d), hd))

    first_round(True)
    mark("rs2c")
    from_twin(1)
    from_twin(3)
    for b in (2, 3):
        xpo[b] = chip_sum(1, b).astype(BF)
        xmo[3 - b] = chip_sum(3, 3 - b).astype(BF)
    for b in (2, 3):
        push(xpo.at[b], xli.at[b], send_s.at[11], far_r.at[1], (me, right))
        push(xmo.at[3 - b], xri.at[3 - b], send_s.at[12], far_r.at[2], (me, left))
    mark("agtwin")
    twin_took(3)
    mark("do3")
    grad_heads((far, other[2]))
    do[...] = dacc[...].astype(BF)
    mark("gwfar")
    grad_weight(2, 0)
    grad_weight(2, 1)

    def second_round():
        for d in range(1, 4):
            push(sa.at[lax.rem(y + d, 4)], ra.at[y], send_s.at[15], gw_r.at[2], (along_y(d), hd))
            push(sb.at[lax.rem(z + d, 4)], rb.at[z], send_s.at[16], gw_r.at[3], (along_z(d), hd))

    def round_wait(dst_a, dst_b, i):
        arrived(dst_a.at[pl.ds(0, 3)], gw_r.at[i])
        arrived(dst_b.at[pl.ds(0, 3)], gw_r.at[i + 1])

    def four(ref):
        return (ref[0].astype(F32) + ref[1].astype(F32)) + (ref[2].astype(F32) + ref[3].astype(F32))

    first_round(False)
    ga[z] = wa[z]
    gb[y] = wb[y]

    mark("bwd1")
    for p in range(NP):
        b, h = divmod(p, NH)
        qb = q_ref[rows_of(b), cols_of(h)]
        kb = k_ref[rows_of(b), cols_of(h)]
        vb = v_ref[rows_of(b), cols_of(h)]
        dob = do[rows_of(b), cols_of(h)]
        dsh = causal(mm_nt(dob, vb)).astype(BF)
        ds[p] = dsh
        dsolved = mm(lanes(dsh, dob, dob), rows(kb, mem_h[p], mem_l[p]))
        dvh, dvl = halves(dsolved)
        dv_h[p] = dvh
        dv_l[p] = dvl
        both = mm_tn(qb, lanes(dvh, dvl))
        dinv = both[:, :HDIM] + both[:, HDIM:]
        dinv = -scale_s[p][:1, :1] * (dinv + dinv.T)
        dt[0, p] = lanes(dinv.astype(BF), jnp.zeros((HDIM, HDIM), BF))
        tan_s[p] = jnp.zeros((HDIM, HDIM), F32)
        both = mm_tn(dob, lanes(sol_h[p], sol_l[p]))
        dm_s[h, b] = both[:, :HDIM] + both[:, HDIM:]

    for h in range(NH):
        pair_sum = (dm_s[h, 0] + dm_s[h, 1]) + (dm_s[h, 2] + dm_s[h, 3])
        pt2[8 * h : 8 * h + 8] = pair_sum.reshape(8, 16, HDIM)
    exchange(pt2, pinbox2, 6)
    pinbox2[me] = pt2[me]

    mark("dual")
    for j in range(NEWTON):
        for p in range(NP):
            high = exh[j, p]
            here = dt[j % 2, p]
            new = mm(lanes(high[:, :HDIM], here[:, :HDIM]), rows(here, high))
            tangent = tan_s[p] + new[:, HDIM:]
            tan_s[p] = tangent
            if j < NEWTON - 1:
                dt[(j + 1) % 2, p] = lanes(new[:, :HDIM].astype(BF), tangent.astype(BF))
            else:
                b, h = divmod(p, NH)
                trace = total(new[:, :HDIM] * unit)
                residual = high_low(exh, exl, p)
                dg_s[h, b] = tangent + (trace * scale_s[p][:1, :1]) * (unit - residual)

    for h in range(NH):
        gram_sum = (dg_s[h, 0] + dg_s[h, 1]) + (dg_s[h, 2] + dg_s[h, 3])
        st2[8 * h : 8 * h + 8] = gram_sum.reshape(8, 16, HDIM).astype(BF)
    exchange(st2, inbox2, 2)
    inbox2[me] = st2[me]

    mark("rs3")
    arrived(x2i, far_r.at[0])
    for b in (0, 1):
        xpo[b] = (chip_sum(1, b) + x2i[b].astype(F32)).astype(BF)
        xmo[3 - b] = (chip_sum(3, 3 - b) + x2i[3 - b].astype(F32)).astype(BF)
    for b in (0, 1):
        push(xpo.at[b], xli.at[b], send_s.at[11], far_r.at[1], (me, right))
        push(xmo.at[3 - b], xri.at[3 - b], send_s.at[12], far_r.at[2], (me, left))

    mark("bwd2")
    for p in range(NP):
        b, h = divmod(p, NH)
        dob = do[rows_of(b), cols_of(h)]
        xh = inv_h[p]
        dvh = dv_h[p]
        gq_ref[rows_of(b), cols_of(h)] = mm(
            lanes(dvh, dv_l[p], dvh), rows(xh, xh, inv_l[p])
        ).astype(BF)
        both = mm_tn(ds[p], lanes(sol_h[p], sol_l[p]))
        own[2, rows_of(b), cols_of(h)] = both[:, :HDIM] + both[:, HDIM:]
        dacc[rows_of(b), cols_of(h)] = mm_tn(sc[p], dob)

    mark("rs4")
    to_twin(0)
    own[0] = partial(0, core)
    send_twin(0)

    mark("pscan")
    exchanged(pinbox2, 6)
    scan(pinbox2, poutb2, reversed(range(CTX)))
    exchange(poutb2, poff2, 7)
    poff2[me] = poutb2[me]

    mark("scan3w")
    exchanged(inbox2, 2)
    mark("scan4s")
    scan(inbox2, outb2, reversed(range(CTX)))
    exchange(outb2, off2, 3)
    off2[me] = outb2[me]

    mark("gw2")
    round_wait(ga, gb, 0)
    for i in range(4):
        sa[i] = ((ga[0, i].astype(F32) + ga[1, i].astype(F32)) + (ga[2, i].astype(F32) + ga[3, i].astype(F32))).astype(BF)
        sb[i] = ((gb[0, i].astype(F32) + gb[1, i].astype(F32)) + (gb[2, i].astype(F32) + gb[3, i].astype(F32))).astype(BF)
    second_round()
    ra[y] = sa[y]
    rb[z] = sb[z]

    mark("scan4w")
    exchanged(poff2, 7)
    exchanged(off2, 3)
    mark("final")
    for h in range(NH):
        gram = off2[8 * h : 8 * h + 8].reshape(HDIM, HDIM).astype(F32)
        pair = poff2[8 * h : 8 * h + 8].reshape(HDIM, HDIM)
        for b in reversed(range(NB)):
            here = rows_of(b)
            kb = k_ref[here, cols_of(h)]
            vb = v_ref[here, cols_of(h)]
            rh, rl = halves(pair)
            dk = own[2, here, cols_of(h)] + mm(lanes(kb, vb, vb), rows(gram.astype(BF), rh, rl))
            gk_ref[here, cols_of(h)] = dk.astype(BF)
            gv_ref[here, cols_of(h)] = (
                dacc[here, cols_of(h)] + mm_nt(lanes(kb, kb), lanes(rh, rl))
            ).astype(BF)
            gram = gram + dg_s[h, b]
            pair = pair + dm_s[h, b]

    mark("gw3")
    round_wait(ra, rb, 2)
    gw_ref[:HDIM, :] = four(ra)
    gw_ref[HDIM:, :] = four(rb)

    mark("lofin")
    from_twin(0)
    arrived(xli, far_r.at[1])
    arrived(xri, far_r.at[2])
    for b in range(NB):
        value = chip_sum(0, b) + xli[b].astype(F32) + xri[b].astype(F32)
        lo_ref[rows_of(b), :] = value.astype(BF)

    mark("waitsend")
    most = pl.ds(0, CTX - 1)
    for i, src in enumerate((st, outb, st2, outb2, pt, poutb, pt2, poutb2)):
        left_here(src.at[most], send_s.at[i])
    left_here(ag.at[pl.ds(0, 7)], send_s.at[8])
    for i, src in enumerate((d2o, x2o, xpo, xmo)):
        left_here(src, send_s.at[9 + i])
    for i, src in enumerate((wa, wb, sa, sb)):
        left_here(src.at[pl.ds(0, 3)], send_s.at[13 + i])
    mark()


def write_out(*refs):
    sources, targets, sems = refs[:5], refs[5:10], refs[10]
    copies = [
        pltpu.make_async_copy(src, dst, sems.at[i])
        for i, (src, dst) in enumerate(zip(sources, targets))
    ]
    for copy in copies:
        copy.start()
    for copy in copies:
        copy.wait()


def shards(queries, keys, values, w_out, cotangent):
    tok = jax.ShapeDtypeStruct((NB * SPAN, NH * HDIM), BF)
    shapes = (tok, tok, tok, tok, jax.ShapeDtypeStruct((256, HDIM), F32))
    vm = lambda *shape: pltpu.VMEM(shape, BF)
    vf = lambda *shape: pltpu.VMEM(shape, F32)
    dma = lambda *shape: pltpu.SemaphoreType.DMA(shape)
    span = pl.BlockSpec(memory_space=pltpu.VMEM)
    anywhere = pl.BlockSpec(memory_space=pl.ANY)
    chunk = [vm(NB, SPAN, 256)]
    flat = [vm(NB * SPAN, 256)]
    scratch = (
        flat * 3 + [vm(256, 2048)] + flat
        + [vm(8, NB, SPAN, 256)]
        + [vf(CTX, 16, HDIM)] * 4 + [vm(CTX, 16, HDIM)] * 4 + [vf(CTX, 16, HDIM)] * 8
        + [vf(NH, NB, HDIM, HDIM)] * 2
        + [vm(NEWTON, NP, HDIM, 256)] * 2
        + [vm(2, NP, HDIM, 256), vf(NP, HDIM, HDIM)]
        + [vf(NP, 8, HDIM)]
        + [vm(NP, HDIM, HDIM)] * 6
        + [vm(NP, SPAN, HDIM)] * 2
        + [vm(NP, SPAN, SPAN)] * 2
        + [vm(NP, SPAN, HDIM)] * 2
        + flat + [vm(256, NB * SPAN), vf(NB * SPAN, 256)] + flat
        + [vf(NH, NB, HDIM, HDIM)] * 2
        + [vm(CHIPS, NB * SPAN, 256)] * 2
        + [vf(CHIPS, NB * SPAN, 256)]
        + chunk * 6
        + [vm(4, 4, HDIM, HDIM)] * 4
        + [vm(4, HDIM, HDIM)] * 4
        + [dma(5)]
        + [dma(17), dma(8), dma(3, NB), dma(4), dma(4), dma(5), dma(3)]
    )
    results = pl.pallas_call(
        kernel,
        out_shape=shapes,
        in_specs=[pl.BlockSpec(memory_space=pltpu.HBM)] * 5,
        out_specs=[span] * 5,
        scratch_shapes=scratch,
        compiler_params=pltpu.CompilerParams(
            collective_id=0, has_side_effects=True, vmem_limit_bytes=VMEM_LIMIT
        ),
        name="mesa_layer",
    )(queries, keys, values, w_out, cotangent)
    return pl.pallas_call(
        write_out,
        out_shape=shapes,
        in_specs=[span] * 5,
        out_specs=[anywhere] * 5,
        scratch_shapes=[dma(5)],
        compiler_params=pltpu.CompilerParams(vmem_limit_bytes=1 * 1024 * 1024),
        name="write_out",
    )(*results)


def solution(mesh):
    placed = (P("ctx", "head"), P("ctx", "head"), P("ctx", "head"), P("head", None), P("ctx", "head"))
    return jax.shard_map(
        shards,
        mesh=mesh,
        in_specs=placed,
        out_specs=(P("ctx", "head"), P("ctx", "head"), P("ctx", "head"), P("ctx", "head"), P("head", "ctx")),
        check_vma=False,
    )
```

```python
import jax
import jax.numpy as jnp
from jax import lax
from jax.experimental import pallas as pl
from jax.experimental.pallas import tpu as pltpu
from jax.sharding import PartitionSpec as P

HDIM = 128
SPAN = 256
NEWTON = 8
RIDGE = 1.0
NB = 4
NH = 2
NP = NB * NH
CTX = 16
CHIPS = 4
VMEM_LIMIT = 103 * 512 * 1024
F32 = jnp.float32
BF = jnp.bfloat16
MESH = pl.DeviceIdType.MESH


def mm(a, b):
    return lax.dot_general(a, b, (((1,), (0,)), ((), ())), preferred_element_type=F32)


def mm_nt(a, b):
    return lax.dot_general(a, b, (((1,), (1,)), ((), ())), preferred_element_type=F32)


def mm_tn(a, b):
    return lax.dot_general(a, b, (((0,), (0,)), ((), ())), preferred_element_type=F32)


def rows(*parts):
    return jnp.concatenate(parts, axis=0)


def lanes(*parts):
    return jnp.concatenate(parts, axis=1)


def halves(value):
    high = value.astype(BF)
    return high, (value - high.astype(F32)).astype(BF)


def total(value):
    return jnp.sum(jnp.sum(value, axis=1, keepdims=True), axis=0, keepdims=True)


def eye():
    shape = (HDIM, HDIM)
    return (
        lax.broadcasted_iota(jnp.int32, shape, 0) == lax.broadcasted_iota(jnp.int32, shape, 1)
    ).astype(F32)


def high_low(high, low, p):
    return high[0, p][:, :HDIM].astype(F32) + low[0, p][:, :HDIM].astype(F32)


def causal(value):
    shape = (SPAN, SPAN)
    keep = lax.broadcasted_iota(jnp.int32, shape, 0) >= lax.broadcasted_iota(jnp.int32, shape, 1)
    return jnp.where(keep, value, 0.0)


def kernel(
    q_hbm, k_hbm, v_hbm, w_hbm, cot_hbm,
    lo_ref, gq_ref, gk_ref, gv_ref, gw_ref,
    q_ref, k_ref, v_ref, w_ref, cot_ref,
    ag, st, inbox, outb, off, st2, inbox2, outb2, off2,
    pt, pinbox, poutb, poff, pt2, pinbox2, poutb2, poff2,
    gram_s, pair_s, exh, exl, dt, tan_s, scale_s, inv_h, inv_l, mem_h, mem_l, memt_h, memt_l,
    sol_h, sol_l, sc, ds, dv_h, dv_l, ho, hot, dacc, do, dg_s, dm_s,
    d2o, d2i, own, x2o, x2i, xpo, xmo, xli, xri, wa, wb, ga, gb, sa, sb, ra, rb,
    in_s, send_s, ex_r, near_r, twin_r, gw_r, d2_r, far_r,
):
    me = lax.axis_index("ctx")
    hd = lax.axis_index("head")
    x = lax.div(hd, 2)
    y = lax.div(me, 4)
    z = lax.rem(me, 4)
    core = lax.rem(hd, 2)
    right = lax.rem(x + 1, CHIPS) * 2 + core
    left = lax.rem(x + 3, CHIPS) * 2 + core
    far = lax.rem(x + 2, CHIPS) * 2 + core
    twin = x * 2 + 1 - core
    other = (left + 1 - 2 * core, right + 1 - 2 * core, far + 1 - 2 * core)
    scope = []

    def mark(name=None):
        if scope:
            scope.pop().__exit__(None, None, None)
        if name is not None:
            now = jax.named_scope(name)
            now.__enter__()
            scope.append(now)

    def remote(src, dst, ss, rs, dev):
        return pltpu.make_async_remote_copy(
            src_ref=src, dst_ref=dst, send_sem=ss, recv_sem=rs, device_id=dev, device_id_type=MESH
        )

    def push(src, dst, ss, rs, dev):
        remote(src, dst, ss, rs, dev).start()

    def arrived(dst, rs):
        remote(dst, dst, send_s.at[0], rs, (me, twin)).wait_recv()

    def left_here(src, ss):
        remote(src, src, ss, ex_r.at[0], (me, twin)).wait_send()

    def exchange(src, dst, i):
        for d in range(1, CTX):
            peer = lax.rem(me + d, CTX)
            push(src.at[peer], dst.at[me], send_s.at[i], ex_r.at[i], (peer, hd))

    def exchanged(dst, i):
        arrived(dst.at[pl.ds(0, CTX - 1)], ex_r.at[i])

    def rows_of(b):
        return slice(b * SPAN, (b + 1) * SPAN)

    def cols_of(h):
        return slice(h * HDIM, (h + 1) * HDIM)

    mark("entry")
    barrier = pltpu.get_barrier_semaphore()
    for d in range(1, CTX):
        pl.semaphore_signal(barrier, inc=1, device_id=(lax.rem(me + d, CTX), hd), device_id_type=MESH)
    for dev in (right, left, twin):
        pl.semaphore_signal(barrier, inc=1, device_id=(me, dev), device_id_type=MESH)
    loads = [
        pltpu.make_async_copy(src, dst, in_s.at[i])
        for i, (src, dst) in enumerate(
            ((k_hbm, k_ref), (v_hbm, v_ref), (cot_hbm, cot_ref), (q_hbm, q_ref), (w_hbm, w_ref))
        )
    ]
    for load in loads[:3]:
        load.start()

    loads[0].wait()
    loads[1].wait()
    for load in loads[3:]:
        load.start()
    mark("gram")
    for h in range(NH):
        gram_sum = jnp.zeros((HDIM, HDIM), F32)
        pair_sum = jnp.zeros((HDIM, HDIM), F32)
        for b in range(NB):
            kb = k_ref[rows_of(b), cols_of(h)]
            vb = v_ref[rows_of(b), cols_of(h)]
            gram = mm_tn(kb, kb)
            pair = mm_tn(vb, kb)
            gram_s[h, b] = gram
            pair_s[h, b] = pair
            gram_sum = gram_sum + gram
            pair_sum = pair_sum + pair
        st[8 * h : 8 * h + 8] = gram_sum.reshape(8, 16, HDIM)
        pt[8 * h : 8 * h + 8] = pair_sum.reshape(8, 16, HDIM)
    inbox[me] = st[me]
    pinbox[me] = pt[me]
    loads[2].wait()
    mark("barrier")
    pl.semaphore_wait(barrier, CTX - 1 + 3)

    exchange(st, inbox, 0)
    for b in range(NB):
        for kind, dev, blk in ((0, right, b), (1, left, (b + 2) % NB)):
            push(
                cot_ref.at[pl.ds(blk * SPAN, SPAN), :], ag.at[hd, blk],
                send_s.at[8], near_r.at[kind, blk], (me, dev),
            )
    for b in range(NB):
        push(
            cot_ref.at[pl.ds(b * SPAN, SPAN), :], ag.at[hd, b],
            send_s.at[8], twin_r.at[0], (me, twin),
        )
        ag[hd, b] = cot_ref[rows_of(b), :]
    exchange(pt, pinbox, 4)

    def take(kind, b, relay=None):
        shard = (left, right, far)[kind]
        here = ag.at[shard, b]
        arrived(here, near_r.at[kind, b])
        if relay is not None:
            push(here, here, send_s.at[8], near_r.at[2, b], (me, relay))
        push(here, here, send_s.at[8], twin_r.at[1 + kind], (me, twin))

    def scan(box, out, order):
        run = jnp.zeros((16, HDIM), F32)
        for i in order:
            out[i] = run.astype(out.dtype)
            run = run + box[i].astype(F32)

    def twin_took(kind):
        arrived(ag.at[(twin, *other)[kind]], twin_r.at[kind])

    def grad_heads(ids, start=False):
        for b in range(NB):
            acc = None if start else dacc[rows_of(b), :]
            for s in ids:
                cols = pl.ds(pl.multiple_of(s * 256, 256), 256)
                part = mm_nt(ag[s, b], w_ref[:, cols])
                acc = part if acc is None else acc + part
            dacc[rows_of(b), :] = acc

    unit = eye()
    loads[3].wait()
    loads[4].wait()
    mark("scan1w")
    exchanged(inbox, 0)
    mark("scan2s")
    scan(inbox, outb, range(CTX))
    exchange(outb, off, 1)
    off[me] = outb[me]
    exchanged(pinbox, 4)
    scan(pinbox, poutb, range(CTX))
    exchange(poutb, poff, 5)
    poff[me] = poutb[me]
    mark("relay")
    take(0, 0, right)
    take(1, 2, left)
    twin_took(0)
    mark("do1")
    grad_heads((hd, twin), True)
    mark("scan2w")
    exchanged(off, 1)

    mark("newton")
    for h in range(NH):
        gram = off[8 * h : 8 * h + 8].reshape(HDIM, HDIM)
        for b in range(NB):
            p = b * NH + h
            ridged = gram + RIDGE * unit
            scale = 1.0 / jnp.sqrt(total(ridged * ridged))
            eh, el = halves(unit - scale * ridged)
            xh, xl = halves(scale * unit)
            exh[0, p] = lanes(eh, xh)
            exl[0, p] = lanes(el, xl)
            scale_s[p] = jnp.broadcast_to(scale, (8, HDIM))
            gram = gram + gram_s[h, b]

    for j in range(NEWTON):
        if j == 3:
            take(0, 1, right)
            take(1, 3, left)
        for p in range(NP):
            high = exh[j, p]
            low = exl[j, p]
            eh = high[:, :HDIM]
            el = low[:, :HDIM]
            if j == NEWTON - 1:
                xh, xl = high[:, HDIM:], low[:, HDIM:]
                new = mm(lanes(eh, el, eh), rows(xh, xh, xl))
                inv_h[p], inv_l[p] = halves(xh.astype(F32) + xl.astype(F32) + new)
                continue
            new = mm(lanes(eh, el, eh), rows(high, high, low))
            iterate = high[:, HDIM:].astype(F32) + low[:, HDIM:].astype(F32) + new[:, HDIM:]
            nh, nl = halves(lanes(new[:, :HDIM], iterate))
            exh[j + 1, p] = nh
            exl[j + 1, p] = nl

    mark("take1")
    take(0, 2)
    take(1, 0)
    mark("pair")
    exchanged(poff, 5)
    for h in range(NH):
        pair = poff[8 * h : 8 * h + 8].reshape(HDIM, HDIM)
        for b in range(NB):
            p = b * NH + h
            mem_h[p], mem_l[p] = halves(pair)
            memt_h[p], memt_l[p] = halves(pair.T)
            pair = pair + pair_s[h, b]

    mark("forward")
    for p in range(NP):
        if p == 5:
            take(0, 3)
            take(1, 1)
        b, h = divmod(p, NH)
        qb = q_ref[rows_of(b), cols_of(h)]
        kb = k_ref[rows_of(b), cols_of(h)]
        vb = v_ref[rows_of(b), cols_of(h)]
        xh = inv_h[p]
        xl = inv_l[p]
        sh, sl = halves(mm(lanes(qb, qb), rows(xh, xl)))
        sol_h[p] = sh
        sol_l[p] = sl
        ch = causal(mm_nt(lanes(sh, sl), lanes(kb, kb))).astype(BF)
        sc[p] = ch
        out = mm(lanes(ch, sh, sh), rows(vb, memt_h[p], memt_l[p]))
        ho[rows_of(b), cols_of(h)] = out.astype(BF)

    def partial(r, c):
        dest = lax.rem(x + r, CHIPS) * 2 + c
        return mm(ho[...], w_ref[:, pl.ds(pl.multiple_of(dest * 256, 256), 256)])

    def to_twin(r):
        d2o[r] = partial(r, 1 - core).astype(BF)

    def send_twin(r):
        push(d2o.at[r], d2i.at[r], send_s.at[9], d2_r.at[r], (me, twin))

    def from_twin(r):
        arrived(d2i.at[r], d2_r.at[r])

    def chip_sum(r, b):
        return own[r, rows_of(b), :] + d2i[r, rows_of(b), :].astype(F32)

    def send_far():
        for i, pair in ((2, (0, 2)), (4, (1, 3))):
            arrived(d2i.at[2, pl.ds(0, 2 * SPAN), :], d2_r.at[i])
            for b in pair:
                x2o[b] = chip_sum(2, b).astype(BF)
            for b in pair:
                push(x2o.at[b], x2i.at[b], send_s.at[10], far_r.at[0], (me, right if b < 2 else left))

    mark("rs1")
    for b in (0, 2, 1, 3):
        dest = lax.rem(x + 2, CHIPS) * 2 + 1 - core
        wcols = w_ref[:, pl.ds(pl.multiple_of(dest * 256, 256), 256)]
        d2o[2, rows_of(b), :] = mm(ho[rows_of(b), :], wcols).astype(BF)
        if b in (2, 3):
            for i in (b - 2, b):
                part = d2o.at[2, pl.ds(i * SPAN, SPAN), :]
                push(part, d2i.at[2, pl.ds(i * SPAN, SPAN), :], send_s.at[9], d2_r.at[2 if b == 2 else 4], (me, twin))
    own[2] = partial(2, core)
    mark("rs2even")
    pl.when(core == 0)(send_far)
    mark("rs1b")
    to_twin(1)
    to_twin(3)
    send_twin(1)
    send_twin(3)
    mark("rs2b")
    own[1] = partial(1, core)
    own[3] = partial(3, core)
    mark("rs2odd")
    pl.when(core == 1)(send_far)
    mark("take2b")
    for kind, b in ((2, 0), (2, 2)):
        take(kind, b)
    mark("take3")
    for kind, b in ((2, 1), (2, 3)):
        take(kind, b)
    mark("take4")
    twin_took(1)
    twin_took(2)
    mark("do2")
    grad_heads((left, right, other[0], other[1]))

    def along_z(d):
        return y * 4 + lax.rem(z + d, 4)

    def along_y(d):
        return lax.rem(y + d, 4) * 4 + z

    def grad_weight(r, c):
        chip = lax.rem(x + r, CHIPS)
        part = mm(hot[...], ag[chip * 2 + c].reshape(NB * SPAN, 256)).astype(BF)
        for i in range(2):
            wa[2 * c + i, chip] = part[:HDIM, cols_of(i)]
            wb[chip, 2 * c + i] = part[HDIM:, cols_of(i)]

    mark("gwpart")
    for b in range(NB):
        hot[:, rows_of(b)] = ho[rows_of(b), :].T
    for r in (0, 1, 3):
        grad_weight(r, 0)
        grad_weight(r, 1)
    far_chip = lax.rem(x + 2, CHIPS)

    def first_round(near):
        for d in range(1, 4):
            dest = lax.rem(y + d, 4)
            for r in (0, 1, 3) if near else (2,):
                chip = lax.rem(x + r, CHIPS)
                push(wa.at[lax.rem(z + d, 4), chip], ga.at[z, chip], send_s.at[13], gw_r.at[0], (along_z(d), hd))

            @pl.when((dest != far_chip) if near else (dest == far_chip))
            def _():
                push(wb.at[dest], gb.at[y], send_s.at[14], gw_r.at[1], (along_y(d), hd))

    first_round(True)
    mark("rs2c")
    from_twin(1)
    from_twin(3)
    for b in (2, 3):
        xpo[b] = chip_sum(1, b).astype(BF)
        xmo[3 - b] = chip_sum(3, 3 - b).astype(BF)
    for b in (2, 3):
        push(xpo.at[b], xli.at[b], send_s.at[11], far_r.at[1], (me, right))
        push(xmo.at[3 - b], xri.at[3 - b], send_s.at[12], far_r.at[2], (me, left))
    mark("agtwin")
    twin_took(3)
    mark("do3")
    grad_heads((far, other[2]))
    do[...] = dacc[...].astype(BF)
    mark("dm")
    for p in range(NP):
        b, h = divmod(p, NH)
        both = mm_tn(do[rows_of(b), cols_of(h)], lanes(sol_h[p], sol_l[p]))
        dm_s[h, b] = both[:, :HDIM] + both[:, HDIM:]
    for h in range(NH):
        pair_sum = (dm_s[h, 0] + dm_s[h, 1]) + (dm_s[h, 2] + dm_s[h, 3])
        pt2[8 * h : 8 * h + 8] = pair_sum.reshape(8, 16, HDIM)
    exchange(pt2, pinbox2, 6)
    pinbox2[me] = pt2[me]

    mark("gwfar")
    grad_weight(2, 0)
    grad_weight(2, 1)

    def second_round():
        for d in range(1, 4):
            push(sa.at[lax.rem(y + d, 4)], ra.at[y], send_s.at[15], gw_r.at[2], (along_y(d), hd))
            push(sb.at[lax.rem(z + d, 4)], rb.at[z], send_s.at[16], gw_r.at[3], (along_z(d), hd))

    def round_wait(dst_a, dst_b, i):
        arrived(dst_a.at[pl.ds(0, 3)], gw_r.at[i])
        arrived(dst_b.at[pl.ds(0, 3)], gw_r.at[i + 1])

    def four(ref):
        return (ref[0].astype(F32) + ref[1].astype(F32)) + (ref[2].astype(F32) + ref[3].astype(F32))

    first_round(False)
    ga[z] = wa[z]
    gb[y] = wb[y]

    mark("bwd1")
    for p in range(NP):
        b, h = divmod(p, NH)
        qb = q_ref[rows_of(b), cols_of(h)]
        kb = k_ref[rows_of(b), cols_of(h)]
        vb = v_ref[rows_of(b), cols_of(h)]
        dob = do[rows_of(b), cols_of(h)]
        dsh = causal(mm_nt(dob, vb)).astype(BF)
        ds[p] = dsh
        dsolved = mm(lanes(dsh, dob, dob), rows(kb, mem_h[p], mem_l[p]))
        dvh, dvl = halves(dsolved)
        dv_h[p] = dvh
        dv_l[p] = dvl
        both = mm_tn(qb, lanes(dvh, dvl))
        dinv = both[:, :HDIM] + both[:, HDIM:]
        dinv = -scale_s[p][:1, :1] * (dinv + dinv.T)
        dt[0, p] = lanes(dinv.astype(BF), jnp.zeros((HDIM, HDIM), BF))
        tan_s[p] = jnp.zeros((HDIM, HDIM), F32)

    mark("dual")
    for j in range(NEWTON):
        for p in range(NP):
            high = exh[j, p]
            here = dt[j % 2, p]
            new = mm(lanes(high[:, :HDIM], here[:, :HDIM]), rows(here, high))
            tangent = tan_s[p] + new[:, HDIM:]
            tan_s[p] = tangent
            if j < NEWTON - 1:
                dt[(j + 1) % 2, p] = lanes(new[:, :HDIM].astype(BF), tangent.astype(BF))
            else:
                b, h = divmod(p, NH)
                trace = total(new[:, :HDIM] * unit)
                residual = high_low(exh, exl, p)
                dg_s[h, b] = tangent + (trace * scale_s[p][:1, :1]) * (unit - residual)

    for h in range(NH):
        gram_sum = (dg_s[h, 0] + dg_s[h, 1]) + (dg_s[h, 2] + dg_s[h, 3])
        st2[8 * h : 8 * h + 8] = gram_sum.reshape(8, 16, HDIM).astype(BF)
    exchange(st2, inbox2, 2)
    inbox2[me] = st2[me]

    mark("rs3")
    arrived(x2i, far_r.at[0])
    for b in (0, 1):
        xpo[b] = (chip_sum(1, b) + x2i[b].astype(F32)).astype(BF)
        xmo[3 - b] = (chip_sum(3, 3 - b) + x2i[3 - b].astype(F32)).astype(BF)
    for b in (0, 1):
        push(xpo.at[b], xli.at[b], send_s.at[11], far_r.at[1], (me, right))
        push(xmo.at[3 - b], xri.at[3 - b], send_s.at[12], far_r.at[2], (me, left))

    mark("bwd2")
    for p in range(NP):
        b, h = divmod(p, NH)
        dob = do[rows_of(b), cols_of(h)]
        xh = inv_h[p]
        dvh = dv_h[p]
        gq_ref[rows_of(b), cols_of(h)] = mm(
            lanes(dvh, dv_l[p], dvh), rows(xh, xh, inv_l[p])
        ).astype(BF)
        both = mm_tn(ds[p], lanes(sol_h[p], sol_l[p]))
        own[2, rows_of(b), cols_of(h)] = both[:, :HDIM] + both[:, HDIM:]
        dacc[rows_of(b), cols_of(h)] = mm_tn(sc[p], dob)

    mark("rs4")
    to_twin(0)
    own[0] = partial(0, core)
    send_twin(0)

    mark("pscan")
    exchanged(pinbox2, 6)
    scan(pinbox2, poutb2, reversed(range(CTX)))
    exchange(poutb2, poff2, 7)
    poff2[me] = poutb2[me]

    mark("scan3w")
    exchanged(inbox2, 2)
    mark("scan4s")
    scan(inbox2, outb2, reversed(range(CTX)))
    exchange(outb2, off2, 3)
    off2[me] = outb2[me]

    mark("gw2")
    round_wait(ga, gb, 0)
    for i in range(4):
        sa[i] = ((ga[0, i].astype(F32) + ga[1, i].astype(F32)) + (ga[2, i].astype(F32) + ga[3, i].astype(F32))).astype(BF)
        sb[i] = ((gb[0, i].astype(F32) + gb[1, i].astype(F32)) + (gb[2, i].astype(F32) + gb[3, i].astype(F32))).astype(BF)
    second_round()
    ra[y] = sa[y]
    rb[z] = sb[z]

    mark("scan4w")
    exchanged(poff2, 7)
    exchanged(off2, 3)
    mark("final")
    for h in range(NH):
        gram = off2[8 * h : 8 * h + 8].reshape(HDIM, HDIM).astype(F32)
        pair = poff2[8 * h : 8 * h + 8].reshape(HDIM, HDIM)
        for b in reversed(range(NB)):
            here = rows_of(b)
            kb = k_ref[here, cols_of(h)]
            vb = v_ref[here, cols_of(h)]
            rh, rl = halves(pair)
            dk = own[2, here, cols_of(h)] + mm(lanes(kb, vb, vb), rows(gram.astype(BF), rh, rl))
            gk_ref[here, cols_of(h)] = dk.astype(BF)
            gv_ref[here, cols_of(h)] = (
                dacc[here, cols_of(h)] + mm_nt(lanes(kb, kb), lanes(rh, rl))
            ).astype(BF)
            gram = gram + dg_s[h, b]
            pair = pair + dm_s[h, b]

    mark("gw3")
    round_wait(ra, rb, 2)
    gw_ref[:HDIM, :] = four(ra)
    gw_ref[HDIM:, :] = four(rb)

    mark("lofin")
    from_twin(0)
    arrived(xli, far_r.at[1])
    arrived(xri, far_r.at[2])
    for b in range(NB):
        value = chip_sum(0, b) + xli[b].astype(F32) + xri[b].astype(F32)
        lo_ref[rows_of(b), :] = value.astype(BF)

    mark("waitsend")
    most = pl.ds(0, CTX - 1)
    for i, src in enumerate((st, outb, st2, outb2, pt, poutb, pt2, poutb2)):
        left_here(src.at[most], send_s.at[i])
    left_here(ag.at[pl.ds(0, 7)], send_s.at[8])
    for i, src in enumerate((d2o, x2o, xpo, xmo)):
        left_here(src, send_s.at[9 + i])
    for i, src in enumerate((wa, wb, sa, sb)):
        left_here(src.at[pl.ds(0, 3)], send_s.at[13 + i])
    mark()


def write_out(*refs):
    sources, targets, sems = refs[:5], refs[5:10], refs[10]
    copies = [
        pltpu.make_async_copy(src, dst, sems.at[i])
        for i, (src, dst) in enumerate(zip(sources, targets))
    ]
    for copy in copies:
        copy.start()
    for copy in copies:
        copy.wait()


def shards(queries, keys, values, w_out, cotangent):
    tok = jax.ShapeDtypeStruct((NB * SPAN, NH * HDIM), BF)
    shapes = (tok, tok, tok, tok, jax.ShapeDtypeStruct((256, HDIM), F32))
    vm = lambda *shape: pltpu.VMEM(shape, BF)
    vf = lambda *shape: pltpu.VMEM(shape, F32)
    dma = lambda *shape: pltpu.SemaphoreType.DMA(shape)
    span = pl.BlockSpec(memory_space=pltpu.VMEM)
    anywhere = pl.BlockSpec(memory_space=pl.ANY)
    chunk = [vm(NB, SPAN, 256)]
    flat = [vm(NB * SPAN, 256)]
    scratch = (
        flat * 3 + [vm(256, 2048)] + flat
        + [vm(8, NB, SPAN, 256)]
        + [vf(CTX, 16, HDIM)] * 4 + [vm(CTX, 16, HDIM)] * 4 + [vf(CTX, 16, HDIM)] * 8
        + [vf(NH, NB, HDIM, HDIM)] * 2
        + [vm(NEWTON, NP, HDIM, 256)] * 2
        + [vm(2, NP, HDIM, 256), vf(NP, HDIM, HDIM)]
        + [vf(NP, 8, HDIM)]
        + [vm(NP, HDIM, HDIM)] * 6
        + [vm(NP, SPAN, HDIM)] * 2
        + [vm(NP, SPAN, SPAN)] * 2
        + [vm(NP, SPAN, HDIM)] * 2
        + flat + [vm(256, NB * SPAN), vf(NB * SPAN, 256)] + flat
        + [vf(NH, NB, HDIM, HDIM)] * 2
        + [vm(CHIPS, NB * SPAN, 256)] * 2
        + [vf(CHIPS, NB * SPAN, 256)]
        + chunk * 6
        + [vm(4, 4, HDIM, HDIM)] * 4
        + [vm(4, HDIM, HDIM)] * 4
        + [dma(5)]
        + [dma(17), dma(8), dma(3, NB), dma(4), dma(4), dma(5), dma(3)]
    )
    results = pl.pallas_call(
        kernel,
        out_shape=shapes,
        in_specs=[pl.BlockSpec(memory_space=pltpu.HBM)] * 5,
        out_specs=[span] * 5,
        scratch_shapes=scratch,
        compiler_params=pltpu.CompilerParams(
            collective_id=0, has_side_effects=True, vmem_limit_bytes=VMEM_LIMIT
        ),
        name="mesa_layer",
    )(queries, keys, values, w_out, cotangent)
    return pl.pallas_call(
        write_out,
        out_shape=shapes,
        in_specs=[span] * 5,
        out_specs=[anywhere] * 5,
        scratch_shapes=[dma(5)],
        compiler_params=pltpu.CompilerParams(vmem_limit_bytes=1 * 1024 * 1024),
        name="write_out",
    )(*results)


def solution(mesh):
    placed = (P("ctx", "head"), P("ctx", "head"), P("ctx", "head"), P("head", None), P("ctx", "head"))
    return jax.shard_map(
        shards,
        mesh=mesh,
        in_specs=placed,
        out_specs=(P("ctx", "head"), P("ctx", "head"), P("ctx", "head"), P("ctx", "head"), P("head", "ctx")),
        check_vma=False,
    )
```
